64 devices in a mesh: dp: 4 (over x, y), tp: 16 (over z, core).
Axes of the slice: x: 2, y: 2, z: 8, core: 2. Of those that a mesh axis runs over, the one named last changes fastest.
The devices are a block of a 4x4x8 slice.
Arguments:
- x: bfloat16 [8, 1024, 2048], P('dp', 'tp'), parts along dimension 0
- k_cache: bfloat16 [8, 8192, 16, 128], P('dp', None, 'tp'), parts along dimension 0
- v_cache: bfloat16 [8, 8192, 16, 128], P('dp', None, 'tp'), parts along dimension 0
- prefix_len: int32 [8], P('dp'), parts along dimension 0
- valid_len: int32 [8], P('dp'), parts along dimension 0
- g_attn: bfloat16 [2048], replicated
- w_q: bfloat16 [2048, 2048], P(None, 'tp')
- b_q: bfloat16 [2048], P('tp')
- w_k: bfloat16 [2048, 2048], P(None, 'tp')
- b_k: bfloat16 [2048], P('tp')
- w_v: bfloat16 [2048, 2048], P(None, 'tp')
- b_v: bfloat16 [2048], P('tp')
- w_o: bfloat16 [2048, 2048], P('tp')
- g_mlp: bfloat16 [2048], replicated
- w_gate: bfloat16 [2048, 11008], P(None, 'tp')
- w_up: bfloat16 [2048, 11008], P(None, 'tp')
- w_down: bfloat16 [11008, 2048], P('tp')
Outputs:
- output 1: bfloat16 [8, 1024, 2048], P('dp', 'tp'), parts along dimension 0
- output 2: bfloat16 [8, 8192, 16, 128], P('dp', None, 'tp'), parts along dimension 0
- output 3: bfloat16 [8, 8192, 16, 128], P('dp', None, 'tp'), parts along dimension 0
There are 4 independent parts. The reference program is written for one: setup_inputs(seed, part) draws one part's arguments, and reference() takes and returns one part's arrays. A program takes and returns all parts, laid end to end along the dimension named above; an argument that names none is the same for every part.
All inputs are finite; a program needn't handle non-finite values.
Results may differ from the reference program's by a relative error of at most 0.02.
Values are sent between devices in bfloat16 or wider.
A program may use at most 768 MiB of HBM per device.

```python
import jax
import jax.numpy as jnp
from jax import lax

REQUESTS = 2
CHUNK_LEN = 1024
CACHE_SLOTS = 8192
MODEL_DIM = 2048
NUM_HEADS = 16
KV_HEADS = 2
KV_STORE = 16
HEAD_DIM = 128
FFN_DIM = 11008

ROPE_THETA = 1.0e6
NORM_EPS = 1.0e-6
GROUP_SIZE = NUM_HEADS // KV_STORE
KV_REPEAT = KV_STORE // KV_HEADS


def draw_lengths(key):
    keys = jax.random.split(key, 4)
    prefix = jax.random.randint(keys[0], (REQUESTS,), 0, CACHE_SLOTS - CHUNK_LEN + 1)
    valid = jax.random.randint(keys[1], (REQUESTS,), 1, CHUNK_LEN + 1)
    req_ids = jnp.arange(REQUESTS)
    longest = jax.random.randint(keys[2], (), 0, REQUESTS)
    fullest = jax.random.randint(keys[3], (), 0, REQUESTS)
    prefix = jnp.where(req_ids == longest, CACHE_SLOTS - CHUNK_LEN, prefix)
    valid = jnp.where(req_ids == fullest, CHUNK_LEN, valid)
    return prefix.astype(jnp.int32), valid.astype(jnp.int32)


def gauss(key, shape, scale):
    return jax.random.normal(key, shape, jnp.float32) * scale


def kv_copies(values, axis):
    return jnp.repeat(values, KV_REPEAT, axis=axis)


def setup_inputs(seed: int = 0, part: int = 0) -> dict:
    shared = jax.random.split(jax.random.key(seed), 12)
    local = jax.random.split(jax.random.fold_in(jax.random.key(seed + 1), part), 5)
    prefix, valid = draw_lengths(local[0])
    q_cols = NUM_HEADS * HEAD_DIM
    kv_cols = KV_STORE * HEAD_DIM
    hidden = gauss(local[1], (REQUESTS, CHUNK_LEN, MODEL_DIM), 1.0)
    k_cache = kv_copies(gauss(local[2], (REQUESTS, CACHE_SLOTS, KV_HEADS, HEAD_DIM), 1.0), 2)
    v_mean = gauss(local[3], (REQUESTS, 1, KV_HEADS, HEAD_DIM), 1.0)
    v_cache = kv_copies(v_mean + gauss(local[4], (REQUESTS, CACHE_SLOTS, KV_HEADS, HEAD_DIM), 1.5), 2)
    w_k = kv_copies(gauss(shared[3], (MODEL_DIM, KV_HEADS, HEAD_DIM), MODEL_DIM ** -0.5), 1)
    b_k = kv_copies(gauss(shared[4], (KV_HEADS, HEAD_DIM), 1.0), 0)
    w_v = kv_copies(gauss(shared[5], (MODEL_DIM, KV_HEADS, HEAD_DIM), MODEL_DIM ** -0.5), 1)
    b_v = kv_copies(gauss(shared[6], (KV_HEADS, HEAD_DIM), 1.0), 0)
    return {
        "x": hidden.astype(jnp.bfloat16),
        "k_cache": k_cache.astype(jnp.bfloat16),
        "v_cache": v_cache.astype(jnp.bfloat16),
        "prefix_len": prefix,
        "valid_len": valid,
        "g_attn": (1.0 + gauss(shared[0], (MODEL_DIM,), 0.3)).astype(jnp.bfloat16),
        "w_q": gauss(shared[1], (MODEL_DIM, q_cols), 1.5 * MODEL_DIM ** -0.5).astype(jnp.bfloat16),
        "b_q": gauss(shared[2], (q_cols,), 1.0).astype(jnp.bfloat16),
        "w_k": w_k.reshape(MODEL_DIM, kv_cols).astype(jnp.bfloat16),
        "b_k": b_k.reshape(kv_cols).astype(jnp.bfloat16),
        "w_v": w_v.reshape(MODEL_DIM, kv_cols).astype(jnp.bfloat16),
        "b_v": b_v.reshape(kv_cols).astype(jnp.bfloat16),
        "w_o": gauss(shared[7], (q_cols, MODEL_DIM), q_cols ** -0.5).astype(jnp.bfloat16),
        "g_mlp": (1.0 + gauss(shared[8], (MODEL_DIM,), 0.3)).astype(jnp.bfloat16),
        "w_gate": gauss(shared[9], (MODEL_DIM, FFN_DIM), MODEL_DIM ** -0.5).astype(jnp.bfloat16),
        "w_up": gauss(shared[10], (MODEL_DIM, FFN_DIM), MODEL_DIM ** -0.5).astype(jnp.bfloat16),
        "w_down": gauss(shared[11], (FFN_DIM, MODEL_DIM), 1.5 * FFN_DIM ** -0.5).astype(jnp.bfloat16),
    }


def rms_norm(hidden, gain):
    wide_vals = hidden.astype(jnp.float32)
    inv_rms = lax.rsqrt(jnp.mean(wide_vals * wide_vals, axis=-1, keepdims=True) + NORM_EPS)
    return (wide_vals * inv_rms * gain.astype(jnp.float32)).astype(jnp.bfloat16)


def rotate_heads(heads, positions):
    half = heads.shape[-1] // 2
    inv_freq = ROPE_THETA ** (-(jnp.arange(half, dtype=jnp.float32) * 2.0) / heads.shape[-1])
    angles = positions.astype(jnp.float32)[..., None] * inv_freq
    cos_t = jnp.cos(angles)[..., None, :]
    sin_t = jnp.sin(angles)[..., None, :]
    wide = heads.astype(jnp.float32)
    first_half = wide[..., :half]
    second_half = wide[..., half:]
    rotated = jnp.concatenate([first_half * cos_t - second_half * sin_t, second_half * cos_t + first_half * sin_t], axis=-1)
    return rotated.astype(jnp.bfloat16)


def project(hidden, weight, bias):
    total = jnp.dot(hidden, weight, preferred_element_type=jnp.float32)
    return (total + bias.astype(jnp.float32)).astype(jnp.bfloat16)


def reference(x, k_cache, v_cache, prefix_len, valid_len, g_attn, w_q, b_q, w_k, b_k, w_v, b_v, w_o, g_mlp, w_gate, w_up, w_down):
    row_ids = jnp.arange(CHUNK_LEN)
    slot_ids = jnp.arange(CACHE_SLOTS)

    def one_request(req_args):
        hidden, k_rows, v_rows, start, count = req_args
        positions = start + row_ids
        normed = rms_norm(hidden, g_attn)
        queries = rotate_heads(project(normed, w_q, b_q).reshape(CHUNK_LEN, NUM_HEADS, HEAD_DIM), positions)
        keys_new = rotate_heads(project(normed, w_k, b_k).reshape(CHUNK_LEN, KV_STORE, HEAD_DIM), positions)
        values_new = project(normed, w_v, b_v).reshape(CHUNK_LEN, KV_STORE, HEAD_DIM)
        keep = (row_ids < count)[:, None, None]
        k_old = lax.dynamic_slice_in_dim(k_rows, start, CHUNK_LEN, axis=0)
        v_old = lax.dynamic_slice_in_dim(v_rows, start, CHUNK_LEN, axis=0)
        k_rows = lax.dynamic_update_slice_in_dim(k_rows, jnp.where(keep, keys_new, k_old), start, axis=0)
        v_rows = lax.dynamic_update_slice_in_dim(v_rows, jnp.where(keep, values_new, v_old), start, axis=0)
        limit = start + jnp.minimum(row_ids, count - 1)
        visible = slot_ids[None, :] <= limit[:, None]
        query_groups = queries.reshape(CHUNK_LEN, KV_STORE, GROUP_SIZE, HEAD_DIM)

        def one_head(head_args):
            q_head, k_head, v_head = head_args
            scores = jnp.einsum("cgd,sd->gcs", q_head.astype(jnp.float32), k_head.astype(jnp.float32)) * HEAD_DIM ** -0.5
            scores = jnp.where(visible[None], scores, -1.0e30)
            attn_probs = jax.nn.softmax(scores, axis=-1).astype(jnp.bfloat16)
            mixed = jnp.einsum("gcs,sd->cgd", attn_probs.astype(jnp.float32), v_head.astype(jnp.float32))
            return mixed.astype(jnp.bfloat16)

        heads_out = lax.map(one_head, (jnp.moveaxis(query_groups, 1, 0), jnp.moveaxis(k_rows, 1, 0), jnp.moveaxis(v_rows, 1, 0)))
        attended = jnp.moveaxis(heads_out, 0, 1).reshape(CHUNK_LEN, NUM_HEADS * HEAD_DIM)
        attn_out = jnp.dot(attended, w_o, preferred_element_type=jnp.float32).astype(jnp.bfloat16)
        resid_mid = (hidden.astype(jnp.float32) + attn_out.astype(jnp.float32)).astype(jnp.bfloat16)
        normed_mlp = rms_norm(resid_mid, g_mlp)
        gate = jnp.dot(normed_mlp, w_gate, preferred_element_type=jnp.float32)
        up_proj = jnp.dot(normed_mlp, w_up, preferred_element_type=jnp.float32)
        hidden_act = (jax.nn.silu(gate) * up_proj).astype(jnp.bfloat16)
        down = jnp.dot(hidden_act, w_down, preferred_element_type=jnp.float32).astype(jnp.bfloat16)
        result = (resid_mid.astype(jnp.float32) + down.astype(jnp.float32)).astype(jnp.bfloat16)
        return result, k_rows, v_rows

    x_out, k_out, v_out = lax.map(one_request, (x, k_cache, v_cache, prefix_len, valid_len))
    return x_out, k_out, v_out
```

```python
import functools
import math

import jax
import jax.numpy as jnp
from jax import lax
from jax.experimental import pallas as pl
from jax.experimental.pallas import tpu as pltpu
from jax.sharding import PartitionSpec as P

ROPE_THETA = 1.0e6
NORM_EPS = 1.0e-6


def rms_norm(hidden, gain):
    wide_vals = hidden.astype(jnp.float32)
    inv_rms = lax.rsqrt(jnp.mean(wide_vals * wide_vals, axis=-1, keepdims=True) + NORM_EPS)
    return (wide_vals * inv_rms * gain.astype(jnp.float32)).astype(jnp.bfloat16)


def rotate_heads(heads, positions):
    half = heads.shape[-1] // 2
    inv_freq = ROPE_THETA ** (-(jnp.arange(half, dtype=jnp.float32) * 2.0) / heads.shape[-1])
    angles = positions.astype(jnp.float32)[..., None] * inv_freq
    cos_t = jnp.cos(angles)[..., None, :]
    sin_t = jnp.sin(angles)[..., None, :]
    wide = heads.astype(jnp.float32)
    first_half = wide[..., :half]
    second_half = wide[..., half:]
    rotated = jnp.concatenate([first_half * cos_t - second_half * sin_t, second_half * cos_t + first_half * sin_t], axis=-1)
    return rotated.astype(jnp.bfloat16)


def project(hidden, weight, bias):
    total = jnp.einsum("rcd,dn->rcn", hidden, weight, preferred_element_type=jnp.float32)
    return (total + bias.astype(jnp.float32)).astype(jnp.bfloat16)


NEG = -1.0e30

def attn_kernel(bq, sub, bk, p_ref, c_ref, q_ref, kn_ref, vn_ref, kc_ref, vc_ref, o_ref, ko_ref, vo_ref, shift, vext, m_s, acc_s):
    r = pl.program_id(0)
    qb = pl.program_id(1)
    slots, d = kc_ref.shape
    n_tok = kn_ref.shape[0]
    win = n_tok + 16
    prefix = p_ref[r]
    valid = c_ref[r]

    @pl.when(qb == 0)
    def _merge():
        start = pl.multiple_of(jnp.minimum((prefix // 16) * 16, slots - win), 16)
        off = prefix - start
        rows = lax.broadcasted_iota(jnp.int32, (win, d), 0) - off
        fresh = (rows >= 0) & (rows < valid)
        for new_ref, old_ref, out_ref in ((kn_ref, kc_ref, ko_ref), (vn_ref, vc_ref, vo_ref)):
            out_ref[...] = old_ref[...]
            shift[pl.ds(16, n_tok), :] = new_ref[...].astype(jnp.float32)
            moved = shift[pl.ds(16 - off, win), :]
            old = old_ref[pl.ds(start, win), :].astype(jnp.float32)
            out_ref[pl.ds(start, win), :] = jnp.where(fresh, moved, old).astype(out_ref.dtype)
        vext[:, :d] = vo_ref[...]
        vext[:, d:] = jnp.ones((slots, d), vext.dtype)

    scale2 = (d ** -0.5) * math.log2(math.e)
    m_s[...] = jnp.full_like(m_s, NEG)
    acc_s[...] = jnp.zeros_like(acc_s)
    row0 = qb * bq
    n_full = (prefix + jnp.minimum(row0, valid - 1) + 1) // bk
    n_all = pl.cdiv(prefix + jnp.minimum(row0 + bq - 1, valid - 1) + 1, bk)

    def step(j, masked):
        base = pl.multiple_of(j * bk, bk)
        keys = ko_ref[pl.ds(base, bk), :]
        vals = vext[pl.ds(base, bk), :]
        for t in range(bq // sub):
            sl = pl.ds(t * sub, sub)
            s = lax.dot_general(q_ref[sl, :], keys, (((1,), (1,)), ((), ())), preferred_element_type=jnp.float32)
            if masked:
                rid = lax.broadcasted_iota(jnp.int32, (sub, 1), 0) + (row0 + t * sub)
                lim = prefix + jnp.minimum(rid, valid - 1) - base
                s = jnp.where(lax.broadcasted_iota(jnp.int32, (sub, bk), 1) <= lim, s, NEG)
            m_prev = m_s[sl, :]
            m_new = jnp.maximum(m_prev, jnp.max(s, axis=1, keepdims=True))
            m_s[sl, :] = m_new
            a = jnp.exp2((m_prev - m_new) * scale2)
            p = jnp.exp2((s - m_new[:, :1]) * scale2).astype(vext.dtype)
            pv = lax.dot_general(p, vals, (((1,), (0,)), ((), ())), preferred_element_type=jnp.float32)
            acc_s[sl, :] = acc_s[sl, :] * jnp.concatenate([a, a], axis=1) + pv

    def full_body(j, _):
        step(j, False)
        return 0

    def edge_body(j, _):
        step(j, True)
        return 0

    lax.fori_loop(0, n_full, full_body, 0)
    lax.fori_loop(n_full, n_all, edge_body, 0)
    o_ref[...] = (acc_s[:, :d] / acc_s[:, d:]).astype(o_ref.dtype)


def attention(q, kn, vn, kc, vc, prefix, valid, bq=1024, sub=128, bk=2048):
    n_req, n_tok, d = q.shape
    slots = kc.shape[1]
    sq = pl.Squeezed()
    tok = pl.BlockSpec((sq, bq, d), lambda r, b, *_: (r, b, 0))
    new = pl.BlockSpec((sq, n_tok, d), lambda r, b, *_: (r, 0, 0))
    cache = pl.BlockSpec((sq, slots, d), lambda r, b, *_: (r, 0, 0))
    return pl.pallas_call(
        functools.partial(attn_kernel, bq, sub, bk),
        grid_spec=pltpu.PrefetchScalarGridSpec(
            num_scalar_prefetch=2,
            grid=(n_req, n_tok // bq),
            in_specs=[tok, new, new, cache, cache],
            out_specs=[tok, cache, cache],
            scratch_shapes=[
                pltpu.VMEM((n_tok + 32, d), jnp.float32),
                pltpu.VMEM((slots, 2 * d), jnp.bfloat16),
                pltpu.VMEM((bq, d), jnp.float32),
                pltpu.VMEM((bq, 2 * d), jnp.float32),
            ],
        ),
        out_shape=[
            jax.ShapeDtypeStruct(q.shape, q.dtype),
            jax.ShapeDtypeStruct(kc.shape, kc.dtype),
            jax.ShapeDtypeStruct(vc.shape, vc.dtype),
        ],
        cost_estimate=pl.CostEstimate(flops=8 * n_req * n_tok * slots * d, bytes_accessed=8 * n_req * slots * d, transcendentals=n_req * n_tok * slots),
        compiler_params=pltpu.CompilerParams(vmem_limit_bytes=56 * 2**20, dimension_semantics=("arbitrary", "arbitrary")),
        name="attend",
    )(prefix, valid, q, kn, vn, kc, vc)


MESH = pl.DeviceIdType.MESH


def remote(src, dst, send, recv, target):
    return pltpu.make_async_remote_copy(src_ref=src, dst_ref=dst, send_sem=send, recv_sem=recv, device_id={"tp": target}, device_id_type=MESH)


def tail_kernel(n_tp, o_hbm, x_ref, g_ref, wo_hbm, wg_hbm, wu_hbm, wd_hbm, out_ref,
                o_v, o_all, wo, wg, wu, wd, x1, rows, sums_in, sums_out, part_in, part_out, kept,
                load_sem, own_sem, o_send, o_recv, ring_send, ring_recv, pair_send, pair_recv, sum_send, sum_recv, part_send, part_recv):
    nz = n_tp // 2
    me = lax.axis_index("tp")
    core = lax.rem(me, 2)
    chip = me // 2
    up = lax.rem(chip + 1, nz) * 2 + core
    down = lax.rem(chip + nz - 1, nz) * 2 + core
    pair = chip * 2 + 1 - core
    towards = (up, down)
    n_req, n_rows, width = x_ref.shape
    d = o_v.shape[-1]

    loads = [pltpu.make_async_copy(s, t, load_sem.at[i]) for i, (s, t) in enumerate(((o_hbm, o_v), (wo_hbm, wo), (wg_hbm, wg), (wu_hbm, wu), (wd_hbm, wd)))]
    for c in loads:
        c.start()

    barrier = pltpu.get_barrier_semaphore()
    for k in range(1, n_tp):
        pl.semaphore_signal(barrier, inc=1, device_id={"tp": lax.rem(me + k, n_tp)}, device_id_type=MESH)
    pl.semaphore_wait(barrier, n_tp - 1)

    loads[0].wait()
    mine = pl.ds(pl.multiple_of(me * d, d), d)
    sends = []
    for k in range(1, n_tp):
        there = lax.rem(me + k, n_tp)
        c = remote(o_v.at[:, pl.ds(pl.multiple_of(there * n_rows, n_rows), n_rows), :], o_all.at[:, :, mine], o_send.at[k], o_recv.at[k], there)
        c.start()
        sends.append(c)
    o_all[:, :, mine] = o_v[:, pl.ds(pl.multiple_of(me * n_rows, n_rows), n_rows), :]
    loads[1].wait()
    for c in sends:
        c.wait_recv()

    mixed = jnp.dot(o_all[...].reshape(n_req * n_rows, width), wo[...], preferred_element_type=jnp.float32).astype(jnp.bfloat16)
    resid = (x_ref[...].reshape(n_req * n_rows, width).astype(jnp.float32) + mixed.astype(jnp.float32)).astype(jnp.bfloat16)
    x1[...] = resid.reshape(x1.shape)
    wide = resid.astype(jnp.float32)
    inv = lax.rsqrt(jnp.mean(wide * wide, axis=-1, keepdims=True) + NORM_EPS)
    normed = (wide * inv * g_ref[...].astype(jnp.float32)).astype(jnp.bfloat16)
    rows[0, :, 0] = normed.reshape(n_req, n_rows, width)

    for i in (2, 3, 4):
        loads[i].wait()

    def ring_copy(s, way):
        return remote(rows.at[s, way, 0], rows.at[s + 1, way, 0], ring_send.at[s, way], ring_recv.at[s + 1, way], towards[way])

    def pair_copy(s, way):
        return remote(rows.at[s, way, 0], rows.at[s, way, 1], pair_send.at[s, way], pair_recv.at[s, way], pair)

    def part_copy(s):
        return remote(part_out.at[s], part_in.at[s], part_send.at[s], part_recv.at[s], pair)

    def sum_copy(s, way):
        return remote(sums_out.at[s, way], sums_in.at[s + 1, way], sum_send.at[s, way], sum_recv.at[s + 1, way], towards[way])

    def step(s, _):
        for way in range(2):
            @pl.when(s > 0)
            def _():
                ring_copy(s - 1, way).wait_recv()

            @pl.when(s < nz - 1)
            def _():
                ring_copy(s, way).start()

            pair_copy(s, way).start()
        for way in range(2):
            pair_copy(s, way).wait_recv()
        lhs = rows[s].reshape(4 * n_rows, width)
        gate = jnp.dot(lhs, wg[...], preferred_element_type=jnp.float32)
        lift = jnp.dot(lhs, wu[...], preferred_element_type=jnp.float32)
        act = (jax.nn.silu(gate) * lift).astype(jnp.bfloat16)
        part = jnp.dot(act, wd[...], preferred_element_type=jnp.float32).reshape(2, 2, n_rows, width)
        part_out[s] = part[:, 1].astype(jnp.bfloat16)
        part_copy(s).start()
        kept[jnp.minimum(s, 1)] = part[:, 0]

        @pl.when(s > 0)
        def _():
            part_copy(s).wait_recv()
            for way in range(2):
                @pl.when(s > 1)
                def _():
                    sum_copy(s - 1, way).wait_recv()
                    sums_out[s, way] = (kept[1, way] + part_in[s, way].astype(jnp.float32) + sums_in[s, way].astype(jnp.float32)).astype(jnp.bfloat16)

                @pl.when(s == 1)
                def _():
                    sums_out[s, way] = (kept[1, way] + part_in[s, way].astype(jnp.float32)).astype(jnp.bfloat16)

                sum_copy(s, way).start()
        return 0

    lax.fori_loop(0, nz, step, 0)

    part_copy(0).wait_recv()
    for way in range(2):
        sum_copy(nz - 1, way).wait_recv()
        total = kept[0, way] + part_in[0, way].astype(jnp.float32) + sums_in[nz, way].astype(jnp.float32)
        out_ref[way] = (x1[way].astype(jnp.float32) + total.astype(jnp.bfloat16).astype(jnp.float32)).astype(jnp.bfloat16)

    for c in sends:
        c.wait_send()
    for s in range(nz):
        part_copy(s).wait_send()
        for way in range(2):
            pair_copy(s, way).wait_send()
            if s < nz - 1:
                ring_copy(s, way).wait_send()
            if s > 0:
                sum_copy(s, way).wait_send()


def tail(n_tp, o, x, gain, w_o, w_gate, w_up, w_down):
    n_req, n_rows, width = x.shape
    ffn = w_gate.shape[1]
    nz = n_tp // 2
    bf = jnp.bfloat16
    any_spec = pl.BlockSpec(memory_space=pl.ANY)
    vm = pl.BlockSpec(memory_space=pltpu.VMEM)
    dma = pltpu.SemaphoreType.DMA
    return pl.pallas_call(
        functools.partial(tail_kernel, n_tp),
        out_shape=jax.ShapeDtypeStruct(x.shape, x.dtype),
        in_specs=[any_spec, vm, vm, any_spec, any_spec, any_spec, any_spec],
        out_specs=vm,
        scratch_shapes=[
            pltpu.VMEM(o.shape, bf),
            pltpu.VMEM((n_req, n_rows, width), bf),
            pltpu.VMEM(w_o.shape, bf),
            pltpu.VMEM(w_gate.shape, bf),
            pltpu.VMEM(w_up.shape, bf),
            pltpu.VMEM(w_down.shape, bf),
            pltpu.VMEM((n_req, n_rows, width), bf),
            pltpu.VMEM((nz, 2, 2, n_rows, width), bf),
            pltpu.VMEM((nz + 1, 2, n_rows, width), bf),
            pltpu.VMEM((nz, 2, n_rows, width), bf),
            pltpu.VMEM((nz, 2, n_rows, width), bf),
            pltpu.VMEM((nz, 2, n_rows, width), bf),
            pltpu.VMEM((2, 2, n_rows, width), jnp.float32),
            dma((5,)), dma, dma((n_tp,)), dma((n_tp,)),
            dma((nz, 2)), dma((nz, 2)), dma((nz, 2)), dma((nz, 2)),
            dma((nz, 2)), dma((nz + 1, 2)), dma((nz,)), dma((nz,)),
        ],
        compiler_params=pltpu.CompilerParams(vmem_limit_bytes=62 * 2**20, collective_id=1, has_side_effects=True),
        cost_estimate=pl.CostEstimate(flops=6 * n_tp * n_req * n_rows * width * ffn, bytes_accessed=20 * 2**20, transcendentals=0),
        name="tail",
    )(o, x, gain.reshape(1, width), w_o, w_gate, w_up, w_down)


def solution(mesh):
    n_tp = mesh.shape["tp"]
    row_spec = P("dp", "tp", None)
    cache_spec = P("dp", None, "tp", None)
    req_spec = P("dp")
    rep_spec = P(None)
    col_spec = P(None, "tp")
    bias_spec = P("tp")
    down_spec = P("tp", None)

    def layer(x_rows, k_cache, v_cache, prefix, valid, g_attn, w_q, b_q, w_k, b_k, w_v, b_v, w_o, g_mlp, w_gate, w_up, w_down):
        normed = rms_norm(x_rows, g_attn)
        normed_full = lax.all_gather(normed, "tp", axis=1, tiled=True)
        n_req, n_tokens = normed_full.shape[0], normed_full.shape[1]
        head_dim = k_cache.shape[-1]
        positions = prefix[:, None] + jnp.arange(n_tokens, dtype=jnp.int32)[None, :]
        q = rotate_heads(project(normed_full, w_q, b_q).reshape(n_req, n_tokens, -1, head_dim), positions)
        k = rotate_heads(project(normed_full, w_k, b_k).reshape(n_req, n_tokens, -1, head_dim), positions)
        v = project(normed_full, w_v, b_v)
        w_o, q = lax.optimization_barrier((w_o, q))
        w_o_full = lax.all_gather(w_o, "tp", axis=0, tiled=True)
        flat = (n_req, -1, head_dim)
        o, k_out, v_out = attention(q.reshape(flat), k.reshape(flat), v, k_cache.reshape(flat), v_cache.reshape(flat), prefix, valid)
        out = tail(n_tp, o, x_rows, g_mlp, w_o_full, w_gate, w_up, w_down)
        return out, k_out.reshape(k_cache.shape), v_out.reshape(v_cache.shape)

    in_specs = (row_spec, cache_spec, cache_spec, req_spec, req_spec, rep_spec, col_spec, bias_spec, col_spec, bias_spec, col_spec, bias_spec, down_spec, rep_spec, col_spec, col_spec, down_spec)
    return jax.shard_map(layer, mesh=mesh, in_specs=in_specs, out_specs=(row_spec, cache_spec, cache_spec), check_vma=False)
```

```python
import functools
import math

import jax
import jax.numpy as jnp
from jax import lax
from jax.experimental import pallas as pl
from jax.experimental.pallas import tpu as pltpu
from jax.sharding import PartitionSpec as P

ROPE_THETA = 1.0e6
NORM_EPS = 1.0e-6


NEG = -1.0e30

def attn_kernel(bq, sub, bk, p_ref, c_ref, q_ref, kn_ref, vn_ref, kc_ref, vc_ref, o_ref, ko_ref, vo_ref, shift, vext, m_s, acc_s):
    r = pl.program_id(0)
    qb = pl.program_id(1)
    slots, d = kc_ref.shape
    n_tok = kn_ref.shape[0]
    win = n_tok + 16
    prefix = p_ref[r]
    valid = c_ref[r]

    @pl.when(qb == 0)
    def _merge():
        start = pl.multiple_of(jnp.minimum((prefix // 16) * 16, slots - win), 16)
        off = prefix - start
        rows = lax.broadcasted_iota(jnp.int32, (win, d), 0) - off
        fresh = (rows >= 0) & (rows < valid)
        for new_ref, old_ref, out_ref in ((kn_ref, kc_ref, ko_ref), (vn_ref, vc_ref, vo_ref)):
            out_ref[...] = old_ref[...]
            shift[pl.ds(16, n_tok), :] = new_ref[...].astype(jnp.float32)
            moved = shift[pl.ds(16 - off, win), :]
            old = old_ref[pl.ds(start, win), :].astype(jnp.float32)
            out_ref[pl.ds(start, win), :] = jnp.where(fresh, moved, old).astype(out_ref.dtype)
        vext[:, :d] = vo_ref[...]
        vext[:, d:] = jnp.ones((slots, d), vext.dtype)

    scale2 = (d ** -0.5) * math.log2(math.e)
    m_s[...] = jnp.full_like(m_s, NEG)
    acc_s[...] = jnp.zeros_like(acc_s)
    row0 = qb * bq
    n_full = (prefix + jnp.minimum(row0, valid - 1) + 1) // bk
    n_all = pl.cdiv(prefix + jnp.minimum(row0 + bq - 1, valid - 1) + 1, bk)

    def step(j, masked):
        base = pl.multiple_of(j * bk, bk)
        keys = ko_ref[pl.ds(base, bk), :]
        vals = vext[pl.ds(base, bk), :]
        for t in range(bq // sub):
            sl = pl.ds(t * sub, sub)
            s = lax.dot_general(q_ref[sl, :], keys, (((1,), (1,)), ((), ())), preferred_element_type=jnp.float32)
            if masked:
                rid = lax.broadcasted_iota(jnp.int32, (sub, 1), 0) + (row0 + t * sub)
                lim = prefix + jnp.minimum(rid, valid - 1) - base
                s = jnp.where(lax.broadcasted_iota(jnp.int32, (sub, bk), 1) <= lim, s, NEG)
            m_prev = m_s[sl, :]
            m_new = jnp.maximum(m_prev, jnp.max(s, axis=1, keepdims=True))
            m_s[sl, :] = m_new
            a = jnp.exp2((m_prev - m_new) * scale2)
            p = jnp.exp2((s - m_new[:, :1]) * scale2).astype(vext.dtype)
            pv = lax.dot_general(p, vals, (((1,), (0,)), ((), ())), preferred_element_type=jnp.float32)
            acc_s[sl, :] = acc_s[sl, :] * jnp.concatenate([a, a], axis=1) + pv

    def full_body(j, _):
        step(j, False)
        return 0

    def edge_body(j, _):
        step(j, True)
        return 0

    lax.fori_loop(0, n_full, full_body, 0)
    lax.fori_loop(n_full, n_all, edge_body, 0)
    o_ref[...] = (acc_s[:, :d] / acc_s[:, d:]).astype(o_ref.dtype)


def attention(q, kn, vn, kc, vc, prefix, valid, bq=1024, sub=128, bk=2048):
    n_req, n_tok, d = q.shape
    slots = kc.shape[1]
    sq = pl.Squeezed()
    tok = pl.BlockSpec((sq, bq, d), lambda r, b, *_: (r, b, 0))
    new = pl.BlockSpec((sq, n_tok, d), lambda r, b, *_: (r, 0, 0))
    cache = pl.BlockSpec((sq, slots, d), lambda r, b, *_: (r, 0, 0))
    return pl.pallas_call(
        functools.partial(attn_kernel, bq, sub, bk),
        grid_spec=pltpu.PrefetchScalarGridSpec(
            num_scalar_prefetch=2,
            grid=(n_req, n_tok // bq),
            in_specs=[tok, new, new, cache, cache],
            out_specs=[tok, cache, cache],
            scratch_shapes=[
                pltpu.VMEM((n_tok + 32, d), jnp.float32),
                pltpu.VMEM((slots, 2 * d), jnp.bfloat16),
                pltpu.VMEM((bq, d), jnp.float32),
                pltpu.VMEM((bq, 2 * d), jnp.float32),
            ],
        ),
        out_shape=[
            jax.ShapeDtypeStruct(q.shape, q.dtype),
            jax.ShapeDtypeStruct(kc.shape, kc.dtype),
            jax.ShapeDtypeStruct(vc.shape, vc.dtype),
        ],
        cost_estimate=pl.CostEstimate(flops=8 * n_req * n_tok * slots * d, bytes_accessed=8 * n_req * slots * d, transcendentals=n_req * n_tok * slots),
        compiler_params=pltpu.CompilerParams(vmem_limit_bytes=56 * 2**20, dimension_semantics=("arbitrary", "arbitrary")),
        name="attend",
    )(prefix, valid, q, kn, vn, kc, vc)


MESH = pl.DeviceIdType.MESH


def remote(src, dst, send, recv, target):
    return pltpu.make_async_remote_copy(src_ref=src, dst_ref=dst, send_sem=send, recv_sem=recv, device_id={"tp": target}, device_id_type=MESH)


def tail_kernel(n_tp, o_hbm, x_ref, g_ref, wo_hbm, wg_hbm, wu_hbm, wd_hbm, out_ref,
                o_v, o_all, wo, wg, wu, wd, x1, rows, sums_in, sums_out, part_in, part_out, kept,
                load_sem, o_send, o_recv, ring_send, ring_recv, pair_send, pair_recv, sum_send, sum_recv, part_send, part_recv):
    nz = n_tp // 2
    me = lax.axis_index("tp")
    core = lax.rem(me, 2)
    chip = me // 2
    up = lax.rem(chip + 1, nz) * 2 + core
    down = lax.rem(chip + nz - 1, nz) * 2 + core
    pair = chip * 2 + 1 - core
    towards = (up, down)
    n_req, n_rows, width = x_ref.shape
    d = o_v.shape[-1]

    loads = [pltpu.make_async_copy(s, t, load_sem.at[i]) for i, (s, t) in enumerate(((o_hbm, o_v), (wo_hbm, wo), (wg_hbm, wg), (wu_hbm, wu), (wd_hbm, wd)))]
    for c in loads:
        c.start()

    barrier = pltpu.get_barrier_semaphore()
    for k in range(1, n_tp):
        pl.semaphore_signal(barrier, inc=1, device_id={"tp": lax.rem(me + k, n_tp)}, device_id_type=MESH)
    pl.semaphore_wait(barrier, n_tp - 1)

    loads[0].wait()
    mine = pl.ds(pl.multiple_of(me * d, d), d)
    sends = []
    for k in range(1, n_tp):
        there = lax.rem(me + k, n_tp)
        c = remote(o_v.at[:, pl.ds(pl.multiple_of(there * n_rows, n_rows), n_rows), :], o_all.at[:, :, mine], o_send.at[k], o_recv.at[k], there)
        c.start()
        sends.append(c)
    o_all[:, :, mine] = o_v[:, pl.ds(pl.multiple_of(me * n_rows, n_rows), n_rows), :]
    loads[1].wait()
    for c in sends:
        c.wait_recv()

    mixed = jnp.dot(o_all[...].reshape(n_req * n_rows, width), wo[...], preferred_element_type=jnp.float32).astype(jnp.bfloat16)
    resid = (x_ref[...].reshape(n_req * n_rows, width).astype(jnp.float32) + mixed.astype(jnp.float32)).astype(jnp.bfloat16)
    x1[...] = resid.reshape(x1.shape)
    wide = resid.astype(jnp.float32)
    inv = lax.rsqrt(jnp.mean(wide * wide, axis=-1, keepdims=True) + NORM_EPS)
    normed = (wide * inv * g_ref[...].astype(jnp.float32)).astype(jnp.bfloat16)
    rows[0, :, 0] = normed.reshape(n_req, n_rows, width)

    for i in (2, 3, 4):
        loads[i].wait()

    def ring_copy(s, way):
        return remote(rows.at[s, way, 0], rows.at[s + 1, way, 0], ring_send.at[s, way], ring_recv.at[s + 1, way], towards[way])

    def pair_copy(s, way):
        return remote(rows.at[s, way, 0], rows.at[s, way, 1], pair_send.at[s, way], pair_recv.at[s, way], pair)

    def part_copy(s):
        return remote(part_out.at[s], part_in.at[s], part_send.at[s], part_recv.at[s], pair)

    def sum_copy(s, way):
        return remote(sums_out.at[s, way], sums_in.at[s + 1, way], sum_send.at[s, way], sum_recv.at[s + 1, way], towards[way])

    def step(s, _):
        for way in range(2):
            @pl.when(s > 0)
            def _():
                ring_copy(s - 1, way).wait_recv()

            @pl.when(s < nz - 1)
            def _():
                ring_copy(s, way).start()

            pair_copy(s, way).start()
        for way in range(2):
            pair_copy(s, way).wait_recv()
        lhs = rows[s].reshape(4 * n_rows, width)
        gate = lax.dot_general(lhs, wg[...], (((1,), (1,)), ((), ())), preferred_element_type=jnp.float32)
        lift = lax.dot_general(lhs, wu[...], (((1,), (1,)), ((), ())), preferred_element_type=jnp.float32)
        act = (jax.nn.silu(gate) * lift).astype(jnp.bfloat16)
        part = jnp.dot(act, wd[...], preferred_element_type=jnp.float32).reshape(2, 2, n_rows, width)
        part_out[s] = part[:, 1].astype(jnp.bfloat16)
        part_copy(s).start()
        kept[jnp.minimum(s, 1)] = part[:, 0]

        @pl.when(s > 0)
        def _():
            part_copy(s).wait_recv()
            for way in range(2):
                @pl.when(s > 1)
                def _():
                    sum_copy(s - 1, way).wait_recv()
                    sums_out[s, way] = (kept[1, way] + part_in[s, way].astype(jnp.float32) + sums_in[s, way].astype(jnp.float32)).astype(jnp.bfloat16)

                @pl.when(s == 1)
                def _():
                    sums_out[s, way] = (kept[1, way] + part_in[s, way].astype(jnp.float32)).astype(jnp.bfloat16)

                sum_copy(s, way).start()
        return 0

    lax.fori_loop(0, nz, step, 0)

    part_copy(0).wait_recv()
    for way in range(2):
        sum_copy(nz - 1, way).wait_recv()
        total = kept[0, way] + part_in[0, way].astype(jnp.float32) + sums_in[nz, way].astype(jnp.float32)
        out_ref[way] = (x1[way].astype(jnp.float32) + total.astype(jnp.bfloat16).astype(jnp.float32)).astype(jnp.bfloat16)

    for c in sends:
        c.wait_send()
    for s in range(nz):
        part_copy(s).wait_send()
        for way in range(2):
            pair_copy(s, way).wait_send()
            if s < nz - 1:
                ring_copy(s, way).wait_send()
            if s > 0:
                sum_copy(s, way).wait_send()


def tail(n_tp, o, x, gain, w_o, w_gate, w_up, w_down):
    n_req, n_rows, width = x.shape
    ffn = w_gate.shape[0]
    nz = n_tp // 2
    bf = jnp.bfloat16
    any_spec = pl.BlockSpec(memory_space=pl.ANY)
    vm = pl.BlockSpec(memory_space=pltpu.VMEM)
    dma = pltpu.SemaphoreType.DMA
    return pl.pallas_call(
        functools.partial(tail_kernel, n_tp),
        out_shape=jax.ShapeDtypeStruct(x.shape, x.dtype),
        in_specs=[any_spec, vm, vm, any_spec, any_spec, any_spec, any_spec],
        out_specs=vm,
        scratch_shapes=[
            pltpu.VMEM(o.shape, bf),
            pltpu.VMEM((n_req, n_rows, width), bf),
            pltpu.VMEM(w_o.shape, bf),
            pltpu.VMEM(w_gate.shape, bf),
            pltpu.VMEM(w_up.shape, bf),
            pltpu.VMEM(w_down.shape, bf),
            pltpu.VMEM((n_req, n_rows, width), bf),
            pltpu.VMEM((nz, 2, 2, n_rows, width), bf),
            pltpu.VMEM((nz + 1, 2, n_rows, width), bf),
            pltpu.VMEM((nz, 2, n_rows, width), bf),
            pltpu.VMEM((nz, 2, n_rows, width), bf),
            pltpu.VMEM((nz, 2, n_rows, width), bf),
            pltpu.VMEM((2, 2, n_rows, width), jnp.float32),
            dma((5,)), dma((n_tp,)), dma((n_tp,)),
            dma((nz, 2)), dma((nz, 2)), dma((nz, 2)), dma((nz, 2)),
            dma((nz, 2)), dma((nz + 1, 2)), dma((nz,)), dma((nz,)),
        ],
        compiler_params=pltpu.CompilerParams(vmem_limit_bytes=62 * 2**20, collective_id=1, has_side_effects=True),
        cost_estimate=pl.CostEstimate(flops=6 * n_tp * n_req * n_rows * width * ffn, bytes_accessed=20 * 2**20, transcendentals=0),
        name="tail",
    )(o, x, gain.reshape(1, width), w_o, w_gate, w_up, w_down)


def front_kernel(n_tp, p_ref, x_ref, g_ref, f_ref, b_ref, wq_hbm, wk_hbm, wv_hbm, q_ref, k_ref, v_ref, w, rows, load_sem, ring_send, ring_recv, pair_send, pair_recv):
    nz = n_tp // 2
    me = lax.axis_index("tp")
    core = lax.rem(me, 2)
    chip = me // 2
    up = lax.rem(chip + 1, nz) * 2 + core
    down = lax.rem(chip + nz - 1, nz) * 2 + core
    pair = chip * 2 + 1 - core
    towards = (up, down)
    n_req, n_rows, width = x_ref.shape
    d = q_ref.shape[-1]

    loads = [pltpu.make_async_copy(s, w.at[:, pl.ds(i * d, d)], load_sem.at[i]) for i, s in enumerate((wq_hbm, wk_hbm, wv_hbm))]
    for c in loads:
        c.start()

    barrier = pltpu.get_barrier_semaphore()
    for there in (up, down, pair):
        pl.semaphore_signal(barrier, inc=1, device_id={"tp": there}, device_id_type=MESH)

    wide = x_ref[...].astype(jnp.float32)
    inv = lax.rsqrt(jnp.mean(wide * wide, axis=-1, keepdims=True) + NORM_EPS)
    rows[0, :, 0] = (wide * inv * g_ref[...].astype(jnp.float32)).astype(jnp.bfloat16)
    pl.semaphore_wait(barrier, 3)

    def ring_copy(s, way):
        return remote(rows.at[s, way, 0], rows.at[s + 1, way, 0], ring_send.at[s, way], ring_recv.at[s + 1, way], towards[way])

    def pair_copy(s, way):
        return remote(rows.at[s, way, 0], rows.at[s, way, 1], pair_send.at[s, way], pair_recv.at[s, way], pair)

    def step(s, _):
        for way in range(2):
            @pl.when(s > 0)
            def _():
                ring_copy(s - 1, way).wait_recv()

            @pl.when(s < nz - 1)
            def _():
                ring_copy(s, way).start()

            pair_copy(s, way).start()

        @pl.when(s == 0)
        def _():
            for c in loads:
                c.wait()

        for way in range(2):
            pair_copy(s, way).wait_recv()
        lhs = rows[s].reshape(4 * n_rows, width)
        total = jnp.dot(lhs, w[...], preferred_element_type=jnp.float32)
        got = (total + b_ref[...].astype(jnp.float32)).astype(jnp.bfloat16)
        sign = jnp.where(lax.broadcasted_iota(jnp.int32, (n_rows, d), 1) < d // 2, -1.0, 1.0)
        for way in range(2):
            home = lax.rem(chip + (nz - s if way == 0 else s), nz)
            for other in range(2):
                off = pl.multiple_of((home * 2 + (core if other == 0 else 1 - core)) * n_rows, n_rows)
                at = pl.ds(off, n_rows)
                spot = (lax.broadcasted_iota(jnp.int32, (n_rows, d), 0) + (p_ref[way] + off)).astype(jnp.float32)
                angle = spot * f_ref[...]
                cos_t = jnp.cos(angle)
                sin_t = jnp.sin(angle) * sign
                mine = got[(way * 2 + other) * n_rows:(way * 2 + other + 1) * n_rows]
                for ref, part in ((q_ref, mine[:, :d]), (k_ref, mine[:, d:2 * d])):
                    part = part.astype(jnp.float32)
                    ref[way, at, :] = (part * cos_t + pltpu.roll(part, d // 2, 1) * sin_t).astype(jnp.bfloat16)
                v_ref[way, at, :] = mine[:, 2 * d:]
        return 0

    lax.fori_loop(0, nz, step, 0)
    for s in range(nz):
        for way in range(2):
            pair_copy(s, way).wait_send()
            if s < nz - 1:
                ring_copy(s, way).wait_send()


def front(n_tp, x, gain, prefix, freq, bias, w_q, w_k, w_v):
    n_req, n_rows, width = x.shape
    d = w_q.shape[1]
    nz = n_tp // 2
    n_tok = n_rows * n_tp
    bf = jnp.bfloat16
    any_spec = pl.BlockSpec(memory_space=pl.ANY)
    vm = pl.BlockSpec(memory_space=pltpu.VMEM)
    dma = pltpu.SemaphoreType.DMA
    made = jax.ShapeDtypeStruct((n_req, n_tok, d), bf)
    return pl.pallas_call(
        functools.partial(front_kernel, n_tp),
        out_shape=[made, made, made],
        in_specs=[pl.BlockSpec(memory_space=pltpu.SMEM), vm, vm, vm, vm, any_spec, any_spec, any_spec],
        out_specs=[vm, vm, vm],
        scratch_shapes=[
            pltpu.VMEM((width, 3 * d), bf),
            pltpu.VMEM((nz, 2, 2, n_rows, width), bf),
            dma((3,)), dma((nz, 2)), dma((nz, 2)), dma((nz, 2)), dma((nz, 2)),
        ],
        compiler_params=pltpu.CompilerParams(vmem_limit_bytes=40 * 2**20, collective_id=2, has_side_effects=True),
        cost_estimate=pl.CostEstimate(flops=6 * n_req * n_tok * width * d, bytes_accessed=4 * 2**20, transcendentals=0),
        name="front",
    )(prefix, x, gain.reshape(1, width), freq, bias, w_q, w_k, w_v)


def solution(mesh):
    n_tp = mesh.shape["tp"]
    row_spec = P("dp", "tp", None)
    cache_spec = P("dp", None, "tp", None)
    req_spec = P("dp")
    rep_spec = P(None)
    col_spec = P(None, "tp")
    bias_spec = P("tp")
    down_spec = P("tp", None)

    def layer(x_rows, k_cache, v_cache, prefix, valid, g_attn, w_q, b_q, w_k, b_k, w_v, b_v, w_o, g_mlp, w_gate, w_up, w_down):
        n_req, head_dim = x_rows.shape[0], k_cache.shape[-1]
        half = jnp.arange(head_dim // 2, dtype=jnp.float32)
        freq = ROPE_THETA ** (-(half * 2.0) / head_dim)
        freq = jnp.concatenate([freq, freq])[None]
        bias = jnp.concatenate([b_q, b_k, b_v])[None]
        q, k, v = front(n_tp, x_rows, g_attn, prefix, freq, bias, w_q, w_k, w_v)
        w_o, q = lax.optimization_barrier((w_o, q))
        w_o_full = lax.all_gather(w_o, "tp", axis=0, tiled=True)
        flat = (n_req, -1, head_dim)
        o, k_out, v_out = attention(q, k, v, k_cache.reshape(flat), v_cache.reshape(flat), prefix, valid)
        out = tail(n_tp, o, x_rows, g_mlp, w_o_full, w_gate.T, w_up.T, w_down)
        return out, k_out.reshape(k_cache.shape), v_out.reshape(v_cache.shape)

    in_specs = (row_spec, cache_spec, cache_spec, req_spec, req_spec, rep_spec, col_spec, bias_spec, col_spec, bias_spec, col_spec, bias_spec, down_spec, rep_spec, col_spec, col_spec, down_spec)
    return jax.shard_map(layer, mesh=mesh, in_specs=in_specs, out_specs=(row_spec, cache_spec, cache_spec), check_vma=False)
```

```python
import functools
import math

import jax
import jax.numpy as jnp
from jax import lax
from jax.experimental import pallas as pl
from jax.experimental.pallas import tpu as pltpu
from jax.sharding import PartitionSpec as P

ROPE_THETA = 1.0e6
NORM_EPS = 1.0e-6


NEG = -1.0e30

def attn_kernel(bq, sub, bk, p_ref, c_ref, q_ref, kn_ref, vn_ref, kc_ref, vc_ref, o_ref, ko_ref, vo_ref, shift, vext, m_s, acc_s):
    r = pl.program_id(0)
    qb = pl.program_id(1)
    slots, d = kc_ref.shape
    n_tok = kn_ref.shape[0]
    win = n_tok + 16
    prefix = p_ref[r]
    valid = c_ref[r]

    @pl.when(qb == 0)
    def _merge():
        start = pl.multiple_of(jnp.minimum((prefix // 16) * 16, slots - win), 16)
        off = prefix - start
        rows = lax.broadcasted_iota(jnp.int32, (win, d), 0) - off
        fresh = (rows >= 0) & (rows < valid)
        for new_ref, old_ref, out_ref in ((kn_ref, kc_ref, ko_ref), (vn_ref, vc_ref, vo_ref)):
            out_ref[...] = old_ref[...]
            shift[pl.ds(16, n_tok), :] = new_ref[...].astype(jnp.float32)
            moved = shift[pl.ds(16 - off, win), :]
            old = old_ref[pl.ds(start, win), :].astype(jnp.float32)
            out_ref[pl.ds(start, win), :] = jnp.where(fresh, moved, old).astype(out_ref.dtype)
        vext[:, :d] = vo_ref[...]
        vext[:, d:] = jnp.ones((slots, d), vext.dtype)

    scale2 = (d ** -0.5) * math.log2(math.e)
    m_s[...] = jnp.full_like(m_s, NEG)
    acc_s[...] = jnp.zeros_like(acc_s)
    row0 = qb * bq
    n_full = (prefix + jnp.minimum(row0, valid - 1) + 1) // bk
    n_all = pl.cdiv(prefix + jnp.minimum(row0 + bq - 1, valid - 1) + 1, bk)

    def step(j, masked):
        base = pl.multiple_of(j * bk, bk)
        keys = ko_ref[pl.ds(base, bk), :]
        vals = vext[pl.ds(base, bk), :]
        for t in range(bq // sub):
            sl = pl.ds(t * sub, sub)
            s = lax.dot_general(q_ref[sl, :], keys, (((1,), (1,)), ((), ())), preferred_element_type=jnp.float32)
            if masked:
                rid = lax.broadcasted_iota(jnp.int32, (sub, 1), 0) + (row0 + t * sub)
                lim = prefix + jnp.minimum(rid, valid - 1) - base
                s = jnp.where(lax.broadcasted_iota(jnp.int32, (sub, bk), 1) <= lim, s, NEG)
            m_prev = m_s[sl, :]
            m_new = jnp.maximum(m_prev, jnp.max(s, axis=1, keepdims=True))
            m_s[sl, :] = m_new
            a = jnp.exp2((m_prev - m_new) * scale2)
            p = jnp.exp2((s - m_new[:, :1]) * scale2).astype(vext.dtype)
            pv = lax.dot_general(p, vals, (((1,), (0,)), ((), ())), preferred_element_type=jnp.float32)
            acc_s[sl, :] = acc_s[sl, :] * jnp.concatenate([a, a], axis=1) + pv

    def full_body(j, _):
        step(j, False)
        return 0

    def edge_body(j, _):
        step(j, True)
        return 0

    lax.fori_loop(0, n_full, full_body, 0)
    lax.fori_loop(n_full, n_all, edge_body, 0)
    o_ref[...] = (acc_s[:, :d] / acc_s[:, d:]).astype(o_ref.dtype)


def attention(q, kn, vn, kc, vc, prefix, valid, bq=1024, sub=128, bk=2048):
    n_req, n_tok, d = q.shape
    slots = kc.shape[1]
    sq = pl.Squeezed()
    tok = pl.BlockSpec((sq, bq, d), lambda r, b, *_: (r, b, 0))
    new = pl.BlockSpec((sq, n_tok, d), lambda r, b, *_: (r, 0, 0))
    cache = pl.BlockSpec((sq, slots, d), lambda r, b, *_: (r, 0, 0))
    return pl.pallas_call(
        functools.partial(attn_kernel, bq, sub, bk),
        grid_spec=pltpu.PrefetchScalarGridSpec(
            num_scalar_prefetch=2,
            grid=(n_req, n_tok // bq),
            in_specs=[tok, new, new, cache, cache],
            out_specs=[tok, cache, cache],
            scratch_shapes=[
                pltpu.VMEM((n_tok + 32, d), jnp.float32),
                pltpu.VMEM((slots, 2 * d), jnp.bfloat16),
                pltpu.VMEM((bq, d), jnp.float32),
                pltpu.VMEM((bq, 2 * d), jnp.float32),
            ],
        ),
        out_shape=[
            jax.ShapeDtypeStruct(q.shape, q.dtype),
            jax.ShapeDtypeStruct(kc.shape, kc.dtype),
            jax.ShapeDtypeStruct(vc.shape, vc.dtype),
        ],
        cost_estimate=pl.CostEstimate(flops=8 * n_req * n_tok * slots * d, bytes_accessed=8 * n_req * slots * d, transcendentals=n_req * n_tok * slots),
        compiler_params=pltpu.CompilerParams(vmem_limit_bytes=56 * 2**20, dimension_semantics=("arbitrary", "arbitrary")),
        name="attend",
    )(prefix, valid, q, kn, vn, kc, vc)


CHUNKS = 2
MESH = pl.DeviceIdType.MESH


def remote(src, dst, send, recv, target):
    return pltpu.make_async_remote_copy(src_ref=src, dst_ref=dst, send_sem=send, recv_sem=recv, device_id={"tp": target}, device_id_type=MESH)


def tail_kernel(n_tp, o_hbm, x_ref, g_ref, wo_hbm, wg_hbm, wu_hbm, wd_hbm, out_ref,
                o_v, o_all, wo, wg, wu, wd, x1, rows, sums_in, sums_out, part_in, part_out, kept,
                load_sem, o_send, o_recv, ring_send, ring_recv, pair_send, pair_recv, sum_send, sum_recv, part_send, part_recv):
    nz = n_tp // 2
    me = lax.axis_index("tp")
    core = lax.rem(me, 2)
    chip = me // 2
    up = lax.rem(chip + 1, nz) * 2 + core
    down = lax.rem(chip + nz - 1, nz) * 2 + core
    pair = chip * 2 + 1 - core
    towards = (up, down)
    n_req, n_rows, width = x_ref.shape
    d = o_v.shape[-1]

    loads = [pltpu.make_async_copy(s, t, load_sem.at[i]) for i, (s, t) in enumerate(((o_hbm, o_v), (wo_hbm, wo), (wg_hbm, wg), (wu_hbm, wu), (wd_hbm, wd)))]
    for c in loads:
        c.start()

    barrier = pltpu.get_barrier_semaphore()
    for k in range(1, n_tp):
        pl.semaphore_signal(barrier, inc=1, device_id={"tp": lax.rem(me + k, n_tp)}, device_id_type=MESH)
    pl.semaphore_wait(barrier, n_tp - 1)

    loads[0].wait()
    mine = pl.ds(pl.multiple_of(me * d, d), d)
    sends = []
    for k in range(1, n_tp):
        there = lax.rem(me + k, n_tp)
        c = remote(o_v.at[:, pl.ds(pl.multiple_of(there * n_rows, n_rows), n_rows), :], o_all.at[:, :, mine], o_send.at[k], o_recv.at[k], there)
        c.start()
        sends.append(c)
    o_all[:, :, mine] = o_v[:, pl.ds(pl.multiple_of(me * n_rows, n_rows), n_rows), :]
    loads[1].wait()
    for c in sends:
        c.wait_recv()

    mixed = jnp.dot(o_all[...].reshape(n_req * n_rows, width), wo[...], preferred_element_type=jnp.float32).astype(jnp.bfloat16)
    resid = (x_ref[...].reshape(n_req * n_rows, width).astype(jnp.float32) + mixed.astype(jnp.float32)).astype(jnp.bfloat16)
    x1[...] = resid.reshape(x1.shape)
    wide = resid.astype(jnp.float32)
    inv = lax.rsqrt(jnp.mean(wide * wide, axis=-1, keepdims=True) + NORM_EPS)
    normed = (wide * inv * g_ref[...].astype(jnp.float32)).astype(jnp.bfloat16)
    rows[0, :, 0] = normed.reshape(n_req, n_rows, width)

    for i in (2, 3, 4):
        loads[i].wait()

    span = n_rows // CHUNKS

    def ring_copy(s, way, h):
        part = pl.ds(h * span, span)
        return remote(rows.at[s, way, 0, part], rows.at[s + 1, way, 0, part], ring_send.at[s, way, h], ring_recv.at[s + 1, way, h], towards[way])

    def pair_copy(s, way):
        return remote(rows.at[s, way, 0], rows.at[s, way, 1], pair_send.at[s, way], pair_recv.at[s, way], pair)

    def part_copy(s):
        return remote(part_out.at[s], part_in.at[s], part_send.at[s], part_recv.at[s], pair)

    def sum_copy(s, way, h):
        part = pl.ds(h * span, span)
        return remote(sums_out.at[s, way, part], sums_in.at[s + 1, way, part], sum_send.at[s, way, h], sum_recv.at[s + 1, way, h], towards[way])

    def step(s, _):
        for h in range(CHUNKS):
            for way in range(2):
                @pl.when(s > 0)
                def _():
                    ring_copy(s - 1, way, h).wait_recv()

                @pl.when(s < nz - 1)
                def _():
                    ring_copy(s, way, h).start()

        for way in range(2):
            pair_copy(s, way).start()
        for way in range(2):
            pair_copy(s, way).wait_recv()
        lhs = rows[s].reshape(4 * n_rows, width)
        gate = lax.dot_general(lhs, wg[...], (((1,), (1,)), ((), ())), preferred_element_type=jnp.float32)
        lift = lax.dot_general(lhs, wu[...], (((1,), (1,)), ((), ())), preferred_element_type=jnp.float32)
        act = (jax.nn.silu(gate) * lift).astype(jnp.bfloat16)
        part = jnp.dot(act, wd[...], preferred_element_type=jnp.float32).reshape(2, 2, n_rows, width)
        part_out[s] = part[:, 1].astype(jnp.bfloat16)
        part_copy(s).start()
        kept[jnp.minimum(s, 1)] = part[:, 0]

        @pl.when(s > 0)
        def _():
            part_copy(s).wait_recv()
            for h in range(CHUNKS):
                part = pl.ds(h * span, span)
                for way in range(2):
                    @pl.when(s > 1)
                    def _():
                        sum_copy(s - 1, way, h).wait_recv()
                        sums_out[s, way, part] = (kept[1, way, part] + part_in[s, way, part].astype(jnp.float32) + sums_in[s, way, part].astype(jnp.float32)).astype(jnp.bfloat16)

                    @pl.when(s == 1)
                    def _():
                        sums_out[s, way, part] = (kept[1, way, part] + part_in[s, way, part].astype(jnp.float32)).astype(jnp.bfloat16)

                    sum_copy(s, way, h).start()
        return 0

    lax.fori_loop(0, nz, step, 0)

    part_copy(0).wait_recv()
    for h in range(CHUNKS):
        part = pl.ds(h * span, span)
        for way in range(2):
            sum_copy(nz - 1, way, h).wait_recv()
            total = kept[0, way, part] + part_in[0, way, part].astype(jnp.float32) + sums_in[nz, way, part].astype(jnp.float32)
            out_ref[way, part] = (x1[way, part].astype(jnp.float32) + total.astype(jnp.bfloat16).astype(jnp.float32)).astype(jnp.bfloat16)

    for c in sends:
        c.wait_send()
    for s in range(nz):
        part_copy(s).wait_send()
        for way in range(2):
            pair_copy(s, way).wait_send()
            if s < nz - 1:
                for h in range(CHUNKS):
                    ring_copy(s, way, h).wait_send()
            if s > 0:
                for h in range(CHUNKS):
                    sum_copy(s, way, h).wait_send()


def tail(n_tp, o, x, gain, w_o, w_gate, w_up, w_down):
    n_req, n_rows, width = x.shape
    ffn = w_gate.shape[0]
    nz = n_tp // 2
    bf = jnp.bfloat16
    any_spec = pl.BlockSpec(memory_space=pl.ANY)
    vm = pl.BlockSpec(memory_space=pltpu.VMEM)
    dma = pltpu.SemaphoreType.DMA
    return pl.pallas_call(
        functools.partial(tail_kernel, n_tp),
        out_shape=jax.ShapeDtypeStruct(x.shape, x.dtype),
        in_specs=[any_spec, vm, vm, any_spec, any_spec, any_spec, any_spec],
        out_specs=vm,
        scratch_shapes=[
            pltpu.VMEM(o.shape, bf),
            pltpu.VMEM((n_req, n_rows, width), bf),
            pltpu.VMEM(w_o.shape, bf),
            pltpu.VMEM(w_gate.shape, bf),
            pltpu.VMEM(w_up.shape, bf),
            pltpu.VMEM(w_down.shape, bf),
            pltpu.VMEM((n_req, n_rows, width), bf),
            pltpu.VMEM((nz, 2, 2, n_rows, width), bf),
            pltpu.VMEM((nz + 1, 2, n_rows, width), bf),
            pltpu.VMEM((nz, 2, n_rows, width), bf),
            pltpu.VMEM((nz, 2, n_rows, width), bf),
            pltpu.VMEM((nz, 2, n_rows, width), bf),
            pltpu.VMEM((2, 2, n_rows, width), jnp.float32),
            dma((5,)), dma((n_tp,)), dma((n_tp,)),
            dma((nz, 2, CHUNKS)), dma((nz, 2, CHUNKS)), dma((nz, 2)), dma((nz, 2)),
            dma((nz, 2, CHUNKS)), dma((nz + 1, 2, CHUNKS)), dma((nz,)), dma((nz,)),
        ],
        compiler_params=pltpu.CompilerParams(vmem_limit_bytes=62 * 2**20, collective_id=1, has_side_effects=True),
        cost_estimate=pl.CostEstimate(flops=6 * n_tp * n_req * n_rows * width * ffn, bytes_accessed=20 * 2**20, transcendentals=0),
        name="tail",
    )(o, x, gain.reshape(1, width), w_o, w_gate, w_up, w_down)


def front_kernel(n_tp, n_dp, p_ref, x_ref, g_ref, f_ref, b_ref, wq_hbm, wk_hbm, wv_hbm, wo_hbm, q_ref, k_ref, v_ref, all_hbm,
                 w, rows, wo, load_sem, ring_send, ring_recv, pair_send, pair_recv, a_send, a_recv, b_send, b_recv, c_send, c_recv):
    nz = n_tp // 2
    me = lax.axis_index("tp")
    core = lax.rem(me, 2)
    chip = me // 2
    up = lax.rem(chip + 1, nz) * 2 + core
    down = lax.rem(chip + nz - 1, nz) * 2 + core
    pair = chip * 2 + 1 - core
    towards = (up, down)
    n_req, n_rows, width = x_ref.shape
    d = q_ref.shape[-1]

    loads = [pltpu.make_async_copy(s, w.at[:, pl.ds(i * d, d)], load_sem.at[i]) for i, s in enumerate((wq_hbm, wk_hbm, wv_hbm))]
    own_load = pltpu.make_async_copy(wo_hbm, wo, load_sem.at[3])
    own_load.start()
    for c in loads:
        c.start()

    group = lax.axis_index("dp")
    barrier = pltpu.get_barrier_semaphore()
    for there in (up, down, pair):
        pl.semaphore_signal(barrier, inc=1, device_id={"tp": there}, device_id_type=MESH)
    for k in range(1, n_dp):
        pl.semaphore_signal(barrier, inc=1, device_id={"dp": lax.rem(group + k, n_dp)}, device_id_type=MESH)

    wide = x_ref[...].astype(jnp.float32)
    inv = lax.rsqrt(jnp.mean(wide * wide, axis=-1, keepdims=True) + NORM_EPS)
    rows[0, :, 0] = (wide * inv * g_ref[...].astype(jnp.float32)).astype(jnp.bfloat16)
    pl.semaphore_wait(barrier, 2 + n_dp)

    n_own = wo.shape[0]
    share = n_own // n_dp
    reach = (nz // 2, (nz - 1) // 2)

    def home_rows(s, way, part, count):
        home = lax.rem(chip + (nz - s if way == 0 else s), nz) * 2 + core
        return pl.ds(pl.multiple_of(home * n_own + part * share, 8), count)

    def a_copy(s, way, src=None):
        at = home_rows(s, way, group, share)
        return remote(all_hbm.at[at] if src is None else src, all_hbm.at[at], a_send.at[s, way], a_recv.at[s + 1, way], towards[way])

    def b_copy(s, way, k):
        at = home_rows(s, way, group, share)
        return pltpu.make_async_remote_copy(src_ref=all_hbm.at[at], dst_ref=all_hbm.at[at], send_sem=b_send.at[s, way, k], recv_sem=b_recv.at[s, way, k],
                                            device_id={"dp": lax.rem(group + k, n_dp)}, device_id_type=MESH)

    def b_wait(s, way, k):
        at = home_rows(s, way, lax.rem(group + n_dp - k, n_dp), share)
        pltpu.make_async_remote_copy(src_ref=all_hbm.at[at], dst_ref=all_hbm.at[at], send_sem=b_send.at[s, way, k], recv_sem=b_recv.at[s, way, k],
                                     device_id={"dp": lax.rem(group + k, n_dp)}, device_id_type=MESH).wait_recv()

    def c_copy(s, way, src=None):
        at = home_rows(s, way, 0, n_own)
        return remote(all_hbm.at[at] if src is None else src, all_hbm.at[at], c_send.at[s, way], c_recv.at[s, way], pair)

    def c_wait(s, way):
        home = lax.rem(chip + (nz - s if way == 0 else s), nz) * 2 + 1 - core
        at = pl.ds(pl.multiple_of(home * n_own, 8), n_own)
        remote(all_hbm.at[at], all_hbm.at[at], c_send.at[s, way], c_recv.at[s, way], pair).wait_recv()

    own_load.wait()
    own_share = wo.at[pl.ds(pl.multiple_of(group * share, 8), share)]
    own_store = pltpu.make_async_copy(wo, all_hbm.at[home_rows(0, 0, 0, n_own)], load_sem.at[3])
    own_store.start()
    c_copy(0, 0, wo).start()

    span = n_rows // CHUNKS

    def ring_copy(s, way, h):
        part = pl.ds(h * span, span)
        return remote(rows.at[s, way, 0, part], rows.at[s + 1, way, 0, part], ring_send.at[s, way, h], ring_recv.at[s + 1, way, h], towards[way])

    def pair_copy(s, way):
        return remote(rows.at[s, way, 0], rows.at[s, way, 1], pair_send.at[s, way], pair_recv.at[s, way], pair)

    def step(s, _):
        for h in range(CHUNKS):
            for way in range(2):
                @pl.when(s > 0)
                def _():
                    ring_copy(s - 1, way, h).wait_recv()

                @pl.when(s < nz - 1)
                def _():
                    ring_copy(s, way, h).start()

        for way in range(2):
            pair_copy(s, way).start()

            @pl.when(s == 0)
            def _():
                a_copy(0, way, own_share).start()

            @pl.when((s > 0) & (s <= reach[way]))
            def _():
                a_copy(s - 1, way).wait_recv()

                @pl.when(s < reach[way])
                def _():
                    a_copy(s, way).start()

                for k in range(1, n_dp):
                    b_copy(s, way, k).start()

        @pl.when(s == 0)
        def _():
            for c in loads:
                c.wait()

        for way in range(2):
            pair_copy(s, way).wait_recv()
        lhs = rows[s].reshape(4 * n_rows, width)
        total = jnp.dot(lhs, w[...], preferred_element_type=jnp.float32)
        got = (total + b_ref[...].astype(jnp.float32)).astype(jnp.bfloat16)
        sign = jnp.where(lax.broadcasted_iota(jnp.int32, (n_rows, d), 1) < d // 2, -1.0, 1.0)
        for way in range(2):
            home = lax.rem(chip + (nz - s if way == 0 else s), nz)
            for other in range(2):
                off = pl.multiple_of((home * 2 + (core if other == 0 else 1 - core)) * n_rows, n_rows)
                at = pl.ds(off, n_rows)
                spot = (lax.broadcasted_iota(jnp.int32, (n_rows, d), 0) + (p_ref[way] + off)).astype(jnp.float32)
                angle = spot * f_ref[...]
                cos_t = jnp.cos(angle)
                sin_t = jnp.sin(angle) * sign
                mine = got[(way * 2 + other) * n_rows:(way * 2 + other + 1) * n_rows]
                for ref, part in ((q_ref, mine[:, :d]), (k_ref, mine[:, d:2 * d])):
                    part = part.astype(jnp.float32)
                    ref[way, at, :] = (part * cos_t + pltpu.roll(part, d // 2, 1) * sin_t).astype(jnp.bfloat16)
                v_ref[way, at, :] = mine[:, 2 * d:]
        return 0

    lax.fori_loop(0, nz, step, 0)

    pieces = [(s, way) for s in range(1, nz // 2 + 1) for way in range(2) if s <= reach[way]]
    for s, way in pieces:
        for k in range(1, n_dp):
            b_wait(s, way, k)
        c_copy(s, way).start()
    own_store.wait()
    c_copy(0, 0, wo).wait_send()
    c_wait(0, 0)
    for way in range(2):
        a_copy(0, way, own_share).wait_send()
    for s, way in pieces:
        c_wait(s, way)
        c_copy(s, way).wait_send()
        for k in range(1, n_dp):
            b_copy(s, way, k).wait_send()
        if s < reach[way]:
            a_copy(s, way).wait_send()
    for s in range(nz):
        for way in range(2):
            pair_copy(s, way).wait_send()
            if s < nz - 1:
                for h in range(CHUNKS):
                    ring_copy(s, way, h).wait_send()


def front(n_tp, n_dp, x, gain, prefix, freq, bias, w_q, w_k, w_v, w_o):
    n_req, n_rows, width = x.shape
    d = w_q.shape[1]
    nz = n_tp // 2
    n_tok = n_rows * n_tp
    bf = jnp.bfloat16
    any_spec = pl.BlockSpec(memory_space=pl.ANY)
    vm = pl.BlockSpec(memory_space=pltpu.VMEM)
    dma = pltpu.SemaphoreType.DMA
    made = jax.ShapeDtypeStruct((n_req, n_tok, d), bf)
    return pl.pallas_call(
        functools.partial(front_kernel, n_tp, n_dp),
        out_shape=[made, made, made, jax.ShapeDtypeStruct((n_tp * d, width), bf)],
        in_specs=[pl.BlockSpec(memory_space=pltpu.SMEM), vm, vm, vm, vm, any_spec, any_spec, any_spec, any_spec],
        out_specs=[vm, vm, vm, any_spec],
        scratch_shapes=[
            pltpu.VMEM((width, 3 * d), bf),
            pltpu.VMEM((nz, 2, 2, n_rows, width), bf),
            pltpu.VMEM(w_o.shape, bf),
            dma((4,)), dma((nz, 2, CHUNKS)), dma((nz, 2, CHUNKS)), dma((nz, 2)), dma((nz, 2)),
            dma((nz, 2)), dma((nz, 2)), dma((nz, 2, n_dp)), dma((nz, 2, n_dp)), dma((nz, 2)), dma((nz, 2)),
        ],
        compiler_params=pltpu.CompilerParams(vmem_limit_bytes=40 * 2**20, collective_id=2, has_side_effects=True),
        cost_estimate=pl.CostEstimate(flops=6 * n_req * n_tok * width * d, bytes_accessed=4 * 2**20, transcendentals=0),
        name="front",
    )(prefix, x, gain.reshape(1, width), freq, bias, w_q, w_k, w_v, w_o)


def solution(mesh):
    n_tp = mesh.shape["tp"]
    row_spec = P("dp", "tp", None)
    cache_spec = P("dp", None, "tp", None)
    req_spec = P("dp")
    rep_spec = P(None)
    col_spec = P(None, "tp")
    bias_spec = P("tp")
    down_spec = P("tp", None)

    def layer(x_rows, k_cache, v_cache, prefix, valid, g_attn, w_q, b_q, w_k, b_k, w_v, b_v, w_o, g_mlp, w_gate, w_up, w_down):
        n_req, head_dim = x_rows.shape[0], k_cache.shape[-1]
        half = jnp.arange(head_dim // 2, dtype=jnp.float32)
        freq = ROPE_THETA ** (-(half * 2.0) / head_dim)
        freq = jnp.concatenate([freq, freq])[None]
        bias = jnp.concatenate([b_q, b_k, b_v])[None]
        q, k, v, w_o_full = front(n_tp, mesh.shape["dp"], x_rows, g_attn, prefix, freq, bias, w_q, w_k, w_v, w_o)
        flat = (n_req, -1, head_dim)
        o, k_out, v_out = attention(q, k, v, k_cache.reshape(flat), v_cache.reshape(flat), prefix, valid)
        out = tail(n_tp, o, x_rows, g_mlp, w_o_full, w_gate.T, w_up.T, w_down)
        return out, k_out.reshape(k_cache.shape), v_out.reshape(v_cache.shape)

    in_specs = (row_spec, cache_spec, cache_spec, req_spec, req_spec, rep_spec, col_spec, bias_spec, col_spec, bias_spec, col_spec, bias_spec, down_spec, rep_spec, col_spec, col_spec, down_spec)
    return jax.shard_map(layer, mesh=mesh, in_specs=in_specs, out_specs=(row_spec, cache_spec, cache_spec), check_vma=False)
```

```python
import functools
import math

import jax
import jax.numpy as jnp
from jax import lax
from jax.experimental import pallas as pl
from jax.experimental.pallas import tpu as pltpu
from jax.sharding import PartitionSpec as P

ROPE_THETA = 1.0e6
NORM_EPS = 1.0e-6


CHUNKS = 2
MESH = pl.DeviceIdType.MESH


def remote(src, dst, send, recv, target):
    return pltpu.make_async_remote_copy(src_ref=src, dst_ref=dst, send_sem=send, recv_sem=recv, device_id={"tp": target}, device_id_type=MESH)


def tail_kernel(n_tp, o_all, x_ref, g_ref, wo_hbm, wg_hbm, wu_hbm, wd_hbm, out_ref,
                wo, wg, wu, wd, x1, rows, sums_in, sums_out, part_in, part_out, kept,
                load_sem, ring_send, ring_recv, pair_send, pair_recv, sum_send, sum_recv, part_send, part_recv):
    nz = n_tp // 2
    me = lax.axis_index("tp")
    core = lax.rem(me, 2)
    chip = me // 2
    up = lax.rem(chip + 1, nz) * 2 + core
    down = lax.rem(chip + nz - 1, nz) * 2 + core
    pair = chip * 2 + 1 - core
    towards = (up, down)
    n_req, n_rows, width = x_ref.shape

    loads = [pltpu.make_async_copy(s, t, load_sem.at[i]) for i, (s, t) in enumerate(((wo_hbm, wo), (wg_hbm, wg), (wu_hbm, wu), (wd_hbm, wd)))]
    for c in loads:
        c.start()

    barrier = pltpu.get_barrier_semaphore()
    for there in (up, down, pair):
        pl.semaphore_signal(barrier, inc=1, device_id={"tp": there}, device_id_type=MESH)

    loads[0].wait()
    mixed = jnp.dot(o_all[...].reshape(n_req * n_rows, width), wo[...], preferred_element_type=jnp.float32).astype(jnp.bfloat16)
    resid = (x_ref[...].reshape(n_req * n_rows, width).astype(jnp.float32) + mixed.astype(jnp.float32)).astype(jnp.bfloat16)
    x1[...] = resid.reshape(x1.shape)
    wide = resid.astype(jnp.float32)
    inv = lax.rsqrt(jnp.mean(wide * wide, axis=-1, keepdims=True) + NORM_EPS)
    normed = (wide * inv * g_ref[...].astype(jnp.float32)).astype(jnp.bfloat16)
    pl.semaphore_wait(barrier, 3)
    rows[0, :, 0] = normed.reshape(n_req, n_rows, width)

    for i in (1, 2, 3):
        loads[i].wait()

    span = n_rows // CHUNKS

    def ring_copy(s, way, h):
        part = pl.ds(h * span, span)
        return remote(rows.at[s, way, 0, part], rows.at[s + 1, way, 0, part], ring_send.at[s, way, h], ring_recv.at[s + 1, way, h], towards[way])

    def pair_copy(s, way):
        return remote(rows.at[s, way, 0], rows.at[s, way, 1], pair_send.at[s, way], pair_recv.at[s, way], pair)

    def part_copy(s):
        return remote(part_out.at[s], part_in.at[s], part_send.at[s], part_recv.at[s], pair)

    def sum_copy(s, way, h):
        part = pl.ds(h * span, span)
        return remote(sums_out.at[s, way, part], sums_in.at[s + 1, way, part], sum_send.at[s, way, h], sum_recv.at[s + 1, way, h], towards[way])

    def step(s, _):
        for h in range(CHUNKS):
            for way in range(2):
                @pl.when(s > 0)
                def _():
                    ring_copy(s - 1, way, h).wait_recv()

                @pl.when(s < nz - 1)
                def _():
                    ring_copy(s, way, h).start()

        for way in range(2):
            pair_copy(s, way).start()
        for way in range(2):
            pair_copy(s, way).wait_recv()
        lhs = rows[s].reshape(4 * n_rows, width)
        gate = lax.dot_general(lhs, wg[...], (((1,), (1,)), ((), ())), preferred_element_type=jnp.float32)
        lift = lax.dot_general(lhs, wu[...], (((1,), (1,)), ((), ())), preferred_element_type=jnp.float32)
        act = (jax.nn.silu(gate) * lift).astype(jnp.bfloat16)
        part = jnp.dot(act, wd[...], preferred_element_type=jnp.float32).reshape(2, 2, n_rows, width)
        part_out[s] = part[:, 1].astype(jnp.bfloat16)
        part_copy(s).start()
        kept[jnp.minimum(s, 1)] = part[:, 0]

        @pl.when(s > 0)
        def _():
            part_copy(s).wait_recv()
            for h in range(CHUNKS):
                part = pl.ds(h * span, span)
                for way in range(2):
                    @pl.when(s > 1)
                    def _():
                        sum_copy(s - 1, way, h).wait_recv()
                        sums_out[s, way, part] = (kept[1, way, part] + part_in[s, way, part].astype(jnp.float32) + sums_in[s, way, part].astype(jnp.float32)).astype(jnp.bfloat16)

                    @pl.when(s == 1)
                    def _():
                        sums_out[s, way, part] = (kept[1, way, part] + part_in[s, way, part].astype(jnp.float32)).astype(jnp.bfloat16)

                    sum_copy(s, way, h).start()
        return 0

    lax.fori_loop(0, nz, step, 0)

    part_copy(0).wait_recv()
    for h in range(CHUNKS):
        part = pl.ds(h * span, span)
        for way in range(2):
            sum_copy(nz - 1, way, h).wait_recv()
            total = kept[0, way, part] + part_in[0, way, part].astype(jnp.float32) + sums_in[nz, way, part].astype(jnp.float32)
            out_ref[way, part] = (x1[way, part].astype(jnp.float32) + total.astype(jnp.bfloat16).astype(jnp.float32)).astype(jnp.bfloat16)

    for s in range(nz):
        part_copy(s).wait_send()
        for way in range(2):
            pair_copy(s, way).wait_send()
            if s < nz - 1:
                for h in range(CHUNKS):
                    ring_copy(s, way, h).wait_send()
            if s > 0:
                for h in range(CHUNKS):
                    sum_copy(s, way, h).wait_send()


def tail(n_tp, o, x, gain, w_o, w_gate, w_up, w_down):
    n_req, n_rows, width = x.shape
    ffn = w_gate.shape[0]
    nz = n_tp // 2
    bf = jnp.bfloat16
    any_spec = pl.BlockSpec(memory_space=pl.ANY)
    vm = pl.BlockSpec(memory_space=pltpu.VMEM)
    dma = pltpu.SemaphoreType.DMA
    return pl.pallas_call(
        functools.partial(tail_kernel, n_tp),
        out_shape=jax.ShapeDtypeStruct(x.shape, x.dtype),
        in_specs=[vm, vm, vm, any_spec, any_spec, any_spec, any_spec],
        out_specs=vm,
        scratch_shapes=[
            pltpu.VMEM(w_o.shape, bf),
            pltpu.VMEM(w_gate.shape, bf),
            pltpu.VMEM(w_up.shape, bf),
            pltpu.VMEM(w_down.shape, bf),
            pltpu.VMEM((n_req, n_rows, width), bf),
            pltpu.VMEM((nz, 2, 2, n_rows, width), bf),
            pltpu.VMEM((nz + 1, 2, n_rows, width), bf),
            pltpu.VMEM((nz, 2, n_rows, width), bf),
            pltpu.VMEM((nz, 2, n_rows, width), bf),
            pltpu.VMEM((nz, 2, n_rows, width), bf),
            pltpu.VMEM((2, 2, n_rows, width), jnp.float32),
            dma((4,)),
            dma((nz, 2, CHUNKS)), dma((nz, 2, CHUNKS)), dma((nz, 2)), dma((nz, 2)),
            dma((nz, 2, CHUNKS)), dma((nz + 1, 2, CHUNKS)), dma((nz,)), dma((nz,)),
        ],
        compiler_params=pltpu.CompilerParams(vmem_limit_bytes=62 * 2**20, collective_id=1, has_side_effects=True),
        cost_estimate=pl.CostEstimate(flops=6 * n_tp * n_req * n_rows * width * ffn, bytes_accessed=20 * 2**20, transcendentals=0),
        name="tail",
    )(o, x, gain.reshape(1, width), w_o, w_gate, w_up, w_down)


NEG = -1.0e30
KEY_BLOCKS = 4


def front_kernel(n_tp, n_dp, p_ref, c_ref, x_ref, g_ref, f_ref, b_ref, wq_hbm, wk_hbm, wv_hbm, wo_hbm, kc_hbm, vc_hbm,
                 o_all, kn_ref, vn_ref, all_hbm, ko_hbm, vo_hbm,
                 w, rows, wo, kc, vc, vext, q_abs, vn_ext, m_abs, acc_abs, q_now, m_now, acc_now, o_v,
                 load_sem, cache_sem, ring_send, ring_recv, pair_send, pair_recv, a_send, a_recv, b_send, b_recv, c_send, c_recv, o_send, o_recv):
    nz = n_tp // 2
    me = lax.axis_index("tp")
    core = lax.rem(me, 2)
    chip = me // 2
    group = lax.axis_index("dp")
    up = lax.rem(chip + 1, nz) * 2 + core
    down = lax.rem(chip + nz - 1, nz) * 2 + core
    pair = chip * 2 + 1 - core
    towards = (up, down)
    n_req, n_rows, width = x_ref.shape
    d = q_abs.shape[-1]
    two = 2 * n_rows
    old = vext.shape[1]
    bf, f32 = jnp.bfloat16, jnp.float32

    own_load = pltpu.make_async_copy(wo_hbm, wo, load_sem.at[3])
    own_load.start()
    loads = [pltpu.make_async_copy(s, w.at[:, pl.ds(i * d, d)], load_sem.at[i]) for i, s in enumerate((wq_hbm, wk_hbm, wv_hbm))]
    for c in loads:
        c.start()
    cache_in = [pltpu.make_async_copy(kc_hbm, kc, cache_sem.at[0]), pltpu.make_async_copy(vc_hbm, vc, cache_sem.at[1])]
    cache_out = [pltpu.make_async_copy(kc, ko_hbm, cache_sem.at[2]), pltpu.make_async_copy(vc, vo_hbm, cache_sem.at[3])]
    for c in cache_in:
        c.start()

    barrier = pltpu.get_barrier_semaphore()
    for k in range(1, n_tp):
        pl.semaphore_signal(barrier, inc=1, device_id={"tp": lax.rem(me + k, n_tp)}, device_id_type=MESH)
    for k in range(1, n_dp):
        pl.semaphore_signal(barrier, inc=1, device_id={"dp": lax.rem(group + k, n_dp)}, device_id_type=MESH)

    wide = x_ref[...].astype(f32)
    inv = lax.rsqrt(jnp.mean(wide * wide, axis=-1, keepdims=True) + NORM_EPS)
    rows[0, :, 0] = (wide * inv * g_ref[...].astype(f32)).astype(bf)
    pl.semaphore_wait(barrier, n_tp + n_dp - 2)

    span = n_rows // CHUNKS

    def ring_copy(s, way, h):
        part = pl.ds(h * span, span)
        return remote(rows.at[s, way, 0, part], rows.at[s + 1, way, 0, part], ring_send.at[s, way, h], ring_recv.at[s + 1, way, h], towards[way])

    def pair_copy(s, way):
        return remote(rows.at[s, way, 0], rows.at[s, way, 1], pair_send.at[s, way], pair_recv.at[s, way], pair)

    n_own = wo.shape[0]
    share = n_own // n_dp
    reach = (nz // 2, (nz - 1) // 2)

    def away(s, way):
        return lax.rem(chip + (nz - s if way == 0 else s), nz)

    def home_rows(s, way, part, count):
        return pl.ds(pl.multiple_of((away(s, way) * 2 + core) * n_own + part * share, 8), count)

    def a_copy(s, way, src=None):
        at = home_rows(s, way, group, share)
        return remote(all_hbm.at[at] if src is None else src, all_hbm.at[at], a_send.at[s, way], a_recv.at[s + 1, way], towards[way])

    def b_copy(s, way, k, owner=None):
        at = home_rows(s, way, group if owner is None else owner, share)
        return pltpu.make_async_remote_copy(src_ref=all_hbm.at[at], dst_ref=all_hbm.at[at], send_sem=b_send.at[s, way, k], recv_sem=b_recv.at[s, way, k],
                                            device_id={"dp": lax.rem(group + k, n_dp)}, device_id_type=MESH)

    def c_copy(s, way, src=None):
        at = home_rows(s, way, 0, n_own)
        return remote(all_hbm.at[at] if src is None else src, all_hbm.at[at], c_send.at[s, way], c_recv.at[s, way], pair)

    def c_wait(s, way):
        at = pl.ds(pl.multiple_of((away(s, way) * 2 + 1 - core) * n_own, 8), n_own)
        remote(all_hbm.at[at], all_hbm.at[at], c_send.at[s, way], c_recv.at[s, way], pair).wait_recv()

    for h in range(CHUNKS):
        for way in range(2):
            ring_copy(0, way, h).start()
    for way in range(2):
        pair_copy(0, way).start()
    own_load.wait()
    own_share = wo.at[pl.ds(pl.multiple_of(group * share, 8), share)]
    own_store = pltpu.make_async_copy(wo, all_hbm.at[home_rows(0, 0, 0, n_own)], load_sem.at[3])
    for way in range(2):
        a_copy(0, way, own_share).start()
    own_store.start()
    c_copy(0, 0, wo).start()

    for i in range(2):
        cache_in[i].wait()
        cache_out[i].start()
    for c in cache_out:
        c.wait()
    tile = 1024
    for r in range(n_req):
        def tidy(t, _):
            at = pl.ds(pl.multiple_of(t * tile, tile), tile)
            there = lax.broadcasted_iota(jnp.int32, (tile, d), 0) + t * tile < p_ref[r]
            first = kc[r, 0:16, :].astype(f32)[0:1]
            kc[r, at, :] = jnp.where(there, kc[r, at, :].astype(f32), first).astype(bf)
            vext[r, at, :d] = jnp.where(there, vc[r, at, :].astype(f32), 0.0).astype(bf)
            vext[r, at, d:] = jnp.where(there, 1.0, 0.0).astype(bf)
            return 0

        lax.fori_loop(0, old // tile, tidy, 0)
    vn_ext[:, :, d:] = jnp.ones((n_req, vn_ext.shape[1], d), bf)
    for c in loads:
        c.wait()

    def tick(s):
        @pl.when(s < nz)
        def _():
            for h in range(CHUNKS):
                for way in range(2):
                    ring_copy(s - 1, way, h).wait_recv()

                    @pl.when(s < nz - 1)
                    def _():
                        ring_copy(s, way, h).start()

            for way in range(2):
                pair_copy(s, way).start()

                @pl.when(s <= reach[way])
                def _():
                    a_copy(s - 1, way).wait_recv()

                    @pl.when(s < reach[way])
                    def _():
                        a_copy(s, way).start()

                    for k in range(1, n_dp):
                        b_copy(s, way, k).start()

    scale2 = (d ** -0.5) * math.log2(math.e)
    block = old // KEY_BLOCKS
    nt = (((1,), (1,)), ((), ()))

    def flash(s, m_prev, acc, vals):
        m_new = jnp.maximum(m_prev, jnp.max(s, axis=1, keepdims=True))
        a = jnp.exp2((m_prev - m_new) * scale2)
        p = jnp.exp2((s - m_new[:, :1]) * scale2).astype(bf)
        return m_new, acc * jnp.concatenate([a, a], axis=1) + jnp.dot(p, vals, preferred_element_type=f32)

    tick(1)

    def two_steps(k, _):
        for t in range(2):
            for way in range(2):
                pair_copy(2 * k + t, way).wait_recv()
        lhs = rows[pl.ds(2 * k, 2)].reshape(8 * n_rows, width)
        total = jnp.dot(lhs, w[...], preferred_element_type=f32)
        got = (total + b_ref[...].astype(f32)).astype(bf)
        sign = jnp.where(lax.broadcasted_iota(jnp.int32, (n_rows, d), 1) < d // 2, -1.0, 1.0)

        def places():
            for t in range(2):
                for way in range(2):
                    for other in range(2):
                        off = pl.multiple_of((away(2 * k + t, way) * 2 + (core if other == 0 else 1 - core)) * n_rows, n_rows)
                        yield t, way, other, off

        for t, way, other, off in places():
            at = pl.ds(off, n_rows)
            spot = (lax.broadcasted_iota(jnp.int32, (n_rows, d), 0) + (p_ref[way] + off)).astype(f32)
            angle = spot * f_ref[...]
            cos_t = jnp.cos(angle)
            sin_t = jnp.sin(angle) * sign
            i = ((t * 2 + way) * 2 + other) * n_rows
            mine = got[i:i + n_rows]
            turned = []
            for part in (mine[:, :d], mine[:, d:2 * d]):
                part = part.astype(f32)
                turned.append((part * cos_t + pltpu.roll(part, d // 2, 1) * sin_t).astype(bf))
            q_abs[way, at, :] = turned[0]
            q_now[way, pl.ds(t * two + other * n_rows, n_rows), :] = turned[0]
            kn_ref[way, at, :] = turned[1]
            vn_ref[way, at, :] = mine[:, 2 * d:]
            vn_ext[way, at, :d] = mine[:, 2 * d:]

        m_now[...] = jnp.full_like(m_now, NEG)
        acc_now[...] = jnp.zeros_like(acc_now)

        def keys(j, _):
            at = pl.ds(pl.multiple_of(j * block, block), block)
            for u in range(2):
                for way in range(2):
                    sl = pl.ds(u * two, two)
                    s = lax.dot_general(q_now[way, sl, :], kc[way, at, :], nt, preferred_element_type=f32)
                    m_now[way, sl, :], acc_now[way, sl, :] = flash(s, m_now[way, sl, :], acc_now[way, sl, :], vext[way, at, :])

            @pl.when(j == KEY_BLOCKS // 2 - 1)
            def _():
                tick(2 * k + 2)

            @pl.when(j == KEY_BLOCKS - 1)
            def _():
                tick(2 * k + 3)
            return 0

        lax.fori_loop(0, KEY_BLOCKS, keys, 0)
        for t, way, other, off in places():
            at = pl.ds(off, n_rows)
            here = pl.ds(t * two + other * n_rows, n_rows)
            m_abs[way, at, :] = m_now[way, here, :]
            acc_abs[way, at, :] = acc_now[way, here, :]
        return 0

    lax.fori_loop(0, nz // 2, two_steps, 0)

    pieces = [(s, way) for s in range(1, nz // 2 + 1) for way in range(2) if s <= reach[way]]
    for s, way in pieces:
        for k in range(1, n_dp):
            b_copy(s, way, k, lax.rem(group + n_dp - k, n_dp)).wait_recv()
        c_copy(s, way).start()

    mine = pl.ds(pl.multiple_of(me * d, d), d)

    def o_copy(i, to):
        home = lax.rem(chip + 1 + i, nz)
        off = pl.multiple_of(home * two + to * n_rows, n_rows)
        return remote(o_v.at[:, pl.ds(off, n_rows), :], o_all.at[:, :, mine], o_send.at[i, to], o_recv.at[i, core], home * 2 + to)

    def own_chunk(i, _):
        home = lax.rem(chip + 1 + i, nz)
        at = pl.ds(pl.multiple_of(home * two, two), two)
        for way in range(2):
            s = lax.dot_general(q_abs[way, at, :], kn_ref[way], nt, preferred_element_type=f32)
            rid = lax.broadcasted_iota(jnp.int32, (two, 1), 0) + home * two
            s = jnp.where(lax.broadcasted_iota(jnp.int32, s.shape, 1) <= jnp.minimum(rid, c_ref[way] - 1), s, NEG)
            m_prev = jnp.where(jnp.full((two, d), p_ref[way], jnp.int32) > 0, m_abs[way, at, :], NEG)
            _, acc = flash(s, m_prev, acc_abs[way, at, :], vn_ext[way])
            o_v[way, at, :] = (acc[:, :d] / acc[:, d:]).astype(bf)
        for to in range(2):
            @pl.when((i < nz - 1) | (core != to))
            def _():
                o_copy(i, to).start()

            @pl.when((i == nz - 1) & (core == to))
            def _():
                o_all[:, :, mine] = o_v[:, pl.ds(pl.multiple_of(home * two + to * n_rows, n_rows), n_rows), :]
        return 0

    lax.fori_loop(0, nz, own_chunk, 0)

    def o_wait(i, _):
        for to in range(2):
            @pl.when((i < nz - 1) | (core != to))
            def _():
                source = lax.rem(chip + 2 * nz - 1 - i, nz) * 2 + to
                spot = pl.ds(pl.multiple_of(source * d, d), d)
                remote(o_v.at[:, pl.ds(0, n_rows), :], o_all.at[:, :, spot], o_send.at[i, to], o_recv.at[i, to], pair).wait_recv()
                o_copy(i, to).wait_send()
        return 0

    lax.fori_loop(0, nz, o_wait, 0)

    own_store.wait()
    c_copy(0, 0, wo).wait_send()
    c_wait(0, 0)
    for way in range(2):
        a_copy(0, way, own_share).wait_send()
    for s, way in pieces:
        c_wait(s, way)
        c_copy(s, way).wait_send()
        for k in range(1, n_dp):
            b_copy(s, way, k).wait_send()
        if s < reach[way]:
            a_copy(s, way).wait_send()
    for s in range(nz):
        for way in range(2):
            pair_copy(s, way).wait_send()
            if s < nz - 1:
                for h in range(CHUNKS):
                    ring_copy(s, way, h).wait_send()


def front(n_tp, n_dp, x, gain, prefix, valid, freq, bias, w_q, w_k, w_v, w_o, k_cache, v_cache):
    n_req, n_rows, width = x.shape
    d = w_q.shape[1]
    nz = n_tp // 2
    n_tok = n_rows * n_tp
    slots = k_cache.shape[1]
    old = slots - n_tok
    bf, f32 = jnp.bfloat16, jnp.float32
    any_spec = pl.BlockSpec(memory_space=pl.ANY)
    sm = pl.BlockSpec(memory_space=pltpu.SMEM)
    vm = pl.BlockSpec(memory_space=pltpu.VMEM)
    dma = pltpu.SemaphoreType.DMA
    made = jax.ShapeDtypeStruct((n_req, n_tok, d), bf)
    cache = jax.ShapeDtypeStruct(k_cache.shape, bf)
    return pl.pallas_call(
        functools.partial(front_kernel, n_tp, n_dp),
        out_shape=[jax.ShapeDtypeStruct(x.shape, bf), made, made, jax.ShapeDtypeStruct((n_tp * d, width), bf), cache, cache],
        in_specs=[sm, sm, vm, vm, vm, vm] + [any_spec] * 6,
        out_specs=[vm, vm, vm, any_spec, any_spec, any_spec],
        scratch_shapes=[
            pltpu.VMEM((width, 3 * d), bf),
            pltpu.VMEM((nz, 2, 2, n_rows, width), bf),
            pltpu.VMEM(w_o.shape, bf),
            pltpu.VMEM(k_cache.shape, bf),
            pltpu.VMEM(k_cache.shape, bf),
            pltpu.VMEM((n_req, old, 2 * d), bf),
            pltpu.VMEM((n_req, n_tok, d), bf),
            pltpu.VMEM((n_req, n_tok, 2 * d), bf),
            pltpu.VMEM((n_req, n_tok, d), f32),
            pltpu.VMEM((n_req, n_tok, 2 * d), f32),
            pltpu.VMEM((n_req, 4 * n_rows, d), bf),
            pltpu.VMEM((n_req, 4 * n_rows, d), f32),
            pltpu.VMEM((n_req, 4 * n_rows, 2 * d), f32),
            pltpu.VMEM((n_req, n_tok, d), bf),
            dma((4,)), dma((4,)), dma((nz, 2, CHUNKS)), dma((nz, 2, CHUNKS)), dma((nz, 2)), dma((nz, 2)),
            dma((nz, 2)), dma((nz, 2)), dma((nz, 2, n_dp)), dma((nz, 2, n_dp)), dma((nz, 2)), dma((nz, 2)),
            dma((nz, 2)), dma((nz, 2)),
        ],
        compiler_params=pltpu.CompilerParams(vmem_limit_bytes=62 * 2**20, collective_id=2, has_side_effects=True),
        cost_estimate=pl.CostEstimate(flops=8 * n_req * n_tok * slots * d, bytes_accessed=20 * 2**20, transcendentals=n_req * n_tok * slots),
        name="front",
    )(prefix, valid, x, gain.reshape(1, width), freq, bias, w_q, w_k, w_v, w_o, k_cache, v_cache)


def patch_kernel(p_ref, c_ref, kn_ref, vn_ref, ki_hbm, vi_hbm, ko_hbm, vo_hbm, window, shift, sems):
    n_req, n_tok, d = kn_ref.shape
    slots = ko_hbm.shape[1]
    win = window.shape[2]
    starts, moves_in, moves_out = [], [], []
    for r in range(n_req):
        start = pl.multiple_of(jnp.minimum((p_ref[r] // 16) * 16, slots - win), 16)
        starts.append(start)
        for i, (src, dst) in enumerate(((ki_hbm, ko_hbm), (vi_hbm, vo_hbm))):
            at = pl.ds(start, win)
            moves_in.append(pltpu.make_async_copy(src.at[r, at], window.at[r, i], sems.at[0, r, i]))
            moves_out.append(pltpu.make_async_copy(window.at[r, i], dst.at[r, at], sems.at[1, r, i]))
    for c in moves_in:
        c.start()
    for r in range(n_req):
        off = p_ref[r] - starts[r]
        at = lax.broadcasted_iota(jnp.int32, (win, d), 0) - off
        fresh = (at >= 0) & (at < c_ref[r])
        for i, new_ref in enumerate((kn_ref, vn_ref)):
            shift[pl.ds(16, n_tok), :] = new_ref[r].astype(jnp.float32)
            moved = shift[pl.ds(16 - off, win), :]
            moves_in[r * 2 + i].wait()
            window[r, i] = jnp.where(fresh, moved, window[r, i].astype(jnp.float32)).astype(window.dtype)
            moves_out[r * 2 + i].start()
    for c in moves_out:
        c.wait()


def patch(prefix, valid, k_new, v_new, k_all, v_all):
    n_req, n_tok, d = k_new.shape
    any_spec = pl.BlockSpec(memory_space=pl.ANY)
    sm = pl.BlockSpec(memory_space=pltpu.SMEM)
    vm = pl.BlockSpec(memory_space=pltpu.VMEM)
    same = jax.ShapeDtypeStruct(k_all.shape, k_all.dtype)
    return pl.pallas_call(
        patch_kernel,
        out_shape=[same, same],
        in_specs=[sm, sm, vm, vm, any_spec, any_spec],
        out_specs=[any_spec, any_spec],
        scratch_shapes=[
            pltpu.VMEM((n_req, 2, n_tok + 16, d), k_all.dtype),
            pltpu.VMEM((n_tok + 32, d), jnp.float32),
            pltpu.SemaphoreType.DMA((2, n_req, 2)),
        ],
        input_output_aliases={4: 0, 5: 1},
        compiler_params=pltpu.CompilerParams(vmem_limit_bytes=62 * 2**20),
        cost_estimate=pl.CostEstimate(flops=10**6, bytes_accessed=4 * 2**20, transcendentals=0),
        name="patch",
    )(prefix, valid, k_new, v_new, k_all, v_all)


def solution(mesh):
    n_tp = mesh.shape["tp"]
    row_spec = P("dp", "tp", None)
    cache_spec = P("dp", None, "tp", None)
    req_spec = P("dp")
    rep_spec = P(None)
    col_spec = P(None, "tp")
    bias_spec = P("tp")
    down_spec = P("tp", None)

    def layer(x_rows, k_cache, v_cache, prefix, valid, g_attn, w_q, b_q, w_k, b_k, w_v, b_v, w_o, g_mlp, w_gate, w_up, w_down):
        n_req, head_dim = x_rows.shape[0], k_cache.shape[-1]
        half = jnp.arange(head_dim // 2, dtype=jnp.float32)
        freq = ROPE_THETA ** (-(half * 2.0) / head_dim)
        freq = jnp.concatenate([freq, freq])[None]
        bias = jnp.concatenate([b_q, b_k, b_v])[None]
        flat = (n_req, -1, head_dim)
        o, k_new, v_new, w_o_full, k_all, v_all = front(n_tp, mesh.shape["dp"], x_rows, g_attn, prefix, valid, freq, bias, w_q, w_k, w_v, w_o, k_cache.reshape(flat), v_cache.reshape(flat))
        k_out, v_out = patch(prefix, valid, k_new, v_new, k_all, v_all)
        out = tail(n_tp, o, x_rows, g_mlp, w_o_full, w_gate.T, w_up.T, w_down)
        return out, k_out.reshape(k_cache.shape), v_out.reshape(v_cache.shape)

    in_specs = (row_spec, cache_spec, cache_spec, req_spec, req_spec, rep_spec, col_spec, bias_spec, col_spec, bias_spec, col_spec, bias_spec, down_spec, rep_spec, col_spec, col_spec, down_spec)
    return jax.shard_map(layer, mesh=mesh, in_specs=in_specs, out_specs=(row_spec, cache_spec, cache_spec), check_vma=False)
```

```python
import functools
import math

import jax
import jax.numpy as jnp
import numpy as np
from jax import lax
from jax.experimental import pallas as pl
from jax.experimental.pallas import tpu as pltpu
from jax.sharding import PartitionSpec as P

ROPE_THETA = 1.0e6
NORM_EPS = 1.0e-6


CHUNKS = 2
MESH = pl.DeviceIdType.MESH


def remote(src, dst, send, recv, target):
    return pltpu.make_async_remote_copy(src_ref=src, dst_ref=dst, send_sem=send, recv_sem=recv, device_id={"tp": target}, device_id_type=MESH)


def tail_kernel(n_tp, o_all, x_ref, g_ref, wo_hbm, wg_hbm, wu_hbm, wd_hbm, out_ref,
                wo, wg, wu, wd, x1, rows, sums_in, sums_out, part_in, part_out, kept,
                load_sem, ring_send, ring_recv, pair_send, pair_recv, sum_send, sum_recv, part_send, part_recv):
    nz = n_tp // 2
    me = lax.axis_index("tp")
    core = lax.rem(me, 2)
    chip = me // 2
    up = lax.rem(chip + 1, nz) * 2 + core
    down = lax.rem(chip + nz - 1, nz) * 2 + core
    pair = chip * 2 + 1 - core
    towards = (up, down)
    n_req, n_rows, width = x_ref.shape

    loads = [pltpu.make_async_copy(s, t, load_sem.at[i]) for i, (s, t) in enumerate(((wo_hbm, wo), (wg_hbm, wg), (wu_hbm, wu), (wd_hbm, wd)))]
    loads[0].start()

    barrier = pltpu.get_barrier_semaphore()
    for there in (up, down, pair):
        pl.semaphore_signal(barrier, inc=1, device_id={"tp": there}, device_id_type=MESH)

    loads[0].wait()
    for c in loads[1:]:
        c.start()
    mixed = jnp.dot(o_all[...].reshape(n_req * n_rows, width), wo[...], preferred_element_type=jnp.float32).astype(jnp.bfloat16)
    resid = (x_ref[...].reshape(n_req * n_rows, width).astype(jnp.float32) + mixed.astype(jnp.float32)).astype(jnp.bfloat16)
    x1[...] = resid.reshape(x1.shape)
    wide = resid.astype(jnp.float32)
    inv = lax.rsqrt(jnp.mean(wide * wide, axis=-1, keepdims=True) + NORM_EPS)
    normed = (wide * inv * g_ref[...].astype(jnp.float32).reshape(1, width)).astype(jnp.bfloat16)
    pl.semaphore_wait(barrier, 3)
    rows[0, :, 0] = normed.reshape(n_req, n_rows, width)

    for i in (1, 2, 3):
        loads[i].wait()

    span = n_rows // CHUNKS

    def ring_copy(s, way, h):
        part = pl.ds(h * span, span)
        return remote(rows.at[s, way, 0, part], rows.at[s + 1, way, 0, part], ring_send.at[s, way, h], ring_recv.at[s + 1, way, h], towards[way])

    def pair_copy(s, way):
        return remote(rows.at[s, way, 0], rows.at[s, way, 1], pair_send.at[s, way], pair_recv.at[s, way], pair)

    def part_copy(s):
        return remote(part_out.at[s], part_in.at[s], part_send.at[s], part_recv.at[s], pair)

    def sum_copy(s, way, h):
        part = pl.ds(h * span, span)
        return remote(sums_out.at[s, way, part], sums_in.at[s + 1, way, part], sum_send.at[s, way, h], sum_recv.at[s + 1, way, h], towards[way])

    def step(s, _):
        for h in range(CHUNKS):
            for way in range(2):
                @pl.when(s > 0)
                def _():
                    ring_copy(s - 1, way, h).wait_recv()

                @pl.when(s < nz - 1)
                def _():
                    ring_copy(s, way, h).start()

        for way in range(2):
            pair_copy(s, way).start()
        for way in range(2):
            pair_copy(s, way).wait_recv()
        lhs = rows[s].reshape(4 * n_rows, width)
        gate = lax.dot_general(lhs, wg[...], (((1,), (1,)), ((), ())), preferred_element_type=jnp.float32)
        lift = lax.dot_general(lhs, wu[...], (((1,), (1,)), ((), ())), preferred_element_type=jnp.float32)
        act = (jax.nn.silu(gate) * lift).astype(jnp.bfloat16)
        part = jnp.dot(act, wd[...], preferred_element_type=jnp.float32).reshape(2, 2, n_rows, width)
        part_out[s] = part[:, 1].astype(jnp.bfloat16)
        part_copy(s).start()
        kept[jnp.minimum(s, 1)] = part[:, 0]

        @pl.when(s > 0)
        def _():
            part_copy(s).wait_recv()
            for h in range(CHUNKS):
                part = pl.ds(h * span, span)
                for way in range(2):
                    @pl.when(s > 1)
                    def _():
                        sum_copy(s - 1, way, h).wait_recv()
                        sums_out[s, way, part] = (kept[1, way, part] + part_in[s, way, part].astype(jnp.float32) + sums_in[s, way, part].astype(jnp.float32)).astype(jnp.bfloat16)

                    @pl.when(s == 1)
                    def _():
                        sums_out[s, way, part] = (kept[1, way, part] + part_in[s, way, part].astype(jnp.float32)).astype(jnp.bfloat16)

                    sum_copy(s, way, h).start()
        return 0

    lax.fori_loop(0, nz, step, 0)

    part_copy(0).wait_recv()
    for h in range(CHUNKS):
        part = pl.ds(h * span, span)
        for way in range(2):
            sum_copy(nz - 1, way, h).wait_recv()
            total = kept[0, way, part] + part_in[0, way, part].astype(jnp.float32) + sums_in[nz, way, part].astype(jnp.float32)
            out_ref[way, part] = (x1[way, part].astype(jnp.float32) + total.astype(jnp.bfloat16).astype(jnp.float32)).astype(jnp.bfloat16)

    for s in range(nz):
        part_copy(s).wait_send()
        for way in range(2):
            pair_copy(s, way).wait_send()
            if s < nz - 1:
                for h in range(CHUNKS):
                    ring_copy(s, way, h).wait_send()
            if s > 0:
                for h in range(CHUNKS):
                    sum_copy(s, way, h).wait_send()


def tail(n_tp, o, x, gain, w_o, w_gate, w_up, w_down):
    n_req, n_rows, width = x.shape
    ffn = w_gate.shape[0]
    nz = n_tp // 2
    bf = jnp.bfloat16
    any_spec = pl.BlockSpec(memory_space=pl.ANY)
    vm = pl.BlockSpec(memory_space=pltpu.VMEM)
    dma = pltpu.SemaphoreType.DMA
    return pl.pallas_call(
        functools.partial(tail_kernel, n_tp),
        out_shape=jax.ShapeDtypeStruct(x.shape, x.dtype),
        in_specs=[vm, vm, vm, any_spec, any_spec, any_spec, any_spec],
        out_specs=vm,
        scratch_shapes=[
            pltpu.VMEM(w_o.shape, bf),
            pltpu.VMEM(w_gate.shape, bf),
            pltpu.VMEM(w_up.shape, bf),
            pltpu.VMEM(w_down.shape, bf),
            pltpu.VMEM((n_req, n_rows, width), bf),
            pltpu.VMEM((nz, 2, 2, n_rows, width), bf),
            pltpu.VMEM((nz + 1, 2, n_rows, width), bf),
            pltpu.VMEM((nz, 2, n_rows, width), bf),
            pltpu.VMEM((nz, 2, n_rows, width), bf),
            pltpu.VMEM((nz, 2, n_rows, width), bf),
            pltpu.VMEM((2, 2, n_rows, width), jnp.float32),
            dma((4,)),
            dma((nz, 2, CHUNKS)), dma((nz, 2, CHUNKS)), dma((nz, 2)), dma((nz, 2)),
            dma((nz, 2, CHUNKS)), dma((nz + 1, 2, CHUNKS)), dma((nz,)), dma((nz,)),
        ],
        compiler_params=pltpu.CompilerParams(vmem_limit_bytes=62 * 2**20, collective_id=1, has_side_effects=True),
        cost_estimate=pl.CostEstimate(flops=6 * n_tp * n_req * n_rows * width * ffn, bytes_accessed=20 * 2**20, transcendentals=0),
        name="tail",
    )(o, x, gain, w_o, w_gate, w_up, w_down)


NEG = -1.0e30
KEY_BLOCKS = 4


def front_kernel(n_tp, n_dp, p_ref, c_ref, x_ref, g_ref, f_ref, bq_ref, bk_ref, bv_ref, wq_hbm, wk_hbm, wv_hbm, wo_hbm, kc_hbm, vc_hbm,
                 o_all, kn_ref, vn_ref, all_hbm,
                 w, rows, wo, kc, vc, vext, q_abs, vn_ext, m_abs, acc_abs, q_now, m_now, acc_now, o_v,
                 load_sem, cache_sem, ring_send, ring_recv, pair_send, pair_recv, a_send, a_recv, b_send, b_recv, c_send, c_recv, o_send, o_recv):
    nz = n_tp // 2
    me = lax.axis_index("tp")
    core = lax.rem(me, 2)
    chip = me // 2
    group = lax.axis_index("dp")
    up = lax.rem(chip + 1, nz) * 2 + core
    down = lax.rem(chip + nz - 1, nz) * 2 + core
    pair = chip * 2 + 1 - core
    towards = (up, down)
    n_req, n_rows, width = x_ref.shape
    d = q_abs.shape[-1]
    two = 2 * n_rows
    old = vext.shape[1]
    bf, f32 = jnp.bfloat16, jnp.float32

    own_load = pltpu.make_async_copy(wo_hbm, wo, load_sem.at[3])
    own_load.start()
    loads = [pltpu.make_async_copy(s, w.at[:, pl.ds(i * d, d)], load_sem.at[i]) for i, s in enumerate((wq_hbm, wk_hbm, wv_hbm))]
    for c in loads:
        c.start()
    cache_in = [pltpu.make_async_copy(s.at[:, pl.ds(0, old)], t, cache_sem.at[i]) for i, (s, t) in enumerate(((kc_hbm, kc), (vc_hbm, vc)))]
    for c in cache_in:
        c.start()

    barrier = pltpu.get_barrier_semaphore()
    for k in range(1, n_tp):
        pl.semaphore_signal(barrier, inc=1, device_id={"tp": lax.rem(me + k, n_tp)}, device_id_type=MESH)
    for k in range(1, n_dp):
        pl.semaphore_signal(barrier, inc=1, device_id={"dp": lax.rem(group + k, n_dp)}, device_id_type=MESH)

    wide = x_ref[...].astype(f32)
    inv = lax.rsqrt(jnp.mean(wide * wide, axis=-1, keepdims=True) + NORM_EPS)
    rows[0, :, 0] = (wide * inv * g_ref[...].astype(f32).reshape(1, width)).astype(bf)
    pl.semaphore_wait(barrier, n_tp + n_dp - 2)

    span = n_rows // CHUNKS

    def ring_copy(s, way, h):
        part = pl.ds(h * span, span)
        return remote(rows.at[s, way, 0, part], rows.at[s + 1, way, 0, part], ring_send.at[s, way, h], ring_recv.at[s + 1, way, h], towards[way])

    def pair_copy(s, way):
        return remote(rows.at[s, way, 0], rows.at[s, way, 1], pair_send.at[s, way], pair_recv.at[s, way], pair)

    n_own = wo.shape[0]
    share = n_own // n_dp
    reach = (nz // 2, (nz - 1) // 2)

    def away(s, way):
        return lax.rem(chip + (nz - s if way == 0 else s), nz)

    def home_rows(s, way, part, count):
        return pl.ds(pl.multiple_of((away(s, way) * 2 + core) * n_own + part * share, 8), count)

    def a_copy(s, way, src=None):
        at = home_rows(s, way, group, share)
        return remote(all_hbm.at[at] if src is None else src, all_hbm.at[at], a_send.at[s, way], a_recv.at[s + 1, way], towards[way])

    def b_copy(s, way, k, owner=None):
        at = home_rows(s, way, group if owner is None else owner, share)
        return pltpu.make_async_remote_copy(src_ref=all_hbm.at[at], dst_ref=all_hbm.at[at], send_sem=b_send.at[s, way, k], recv_sem=b_recv.at[s, way, k],
                                            device_id={"dp": lax.rem(group + k, n_dp)}, device_id_type=MESH)

    def c_copy(s, way, src=None):
        at = home_rows(s, way, 0, n_own)
        return remote(all_hbm.at[at] if src is None else src, all_hbm.at[at], c_send.at[s, way], c_recv.at[s, way], pair)

    def c_wait(s, way):
        at = pl.ds(pl.multiple_of((away(s, way) * 2 + 1 - core) * n_own, 8), n_own)
        remote(all_hbm.at[at], all_hbm.at[at], c_send.at[s, way], c_recv.at[s, way], pair).wait_recv()

    for h in range(CHUNKS):
        for way in range(2):
            ring_copy(0, way, h).start()
    for way in range(2):
        pair_copy(0, way).start()
    own_load.wait()
    own_share = wo.at[pl.ds(pl.multiple_of(group * share, 8), share)]
    own_store = pltpu.make_async_copy(wo, all_hbm.at[home_rows(0, 0, 0, n_own)], load_sem.at[3])
    for way in range(2):
        a_copy(0, way, own_share).start()
    own_store.start()
    c_copy(0, 0, wo).start()

    for c in cache_in:
        c.wait()
    tile = 1024
    for r in range(n_req):
        def tidy(t, _):
            at = pl.ds(pl.multiple_of(t * tile, tile), tile)
            there = lax.broadcasted_iota(jnp.int32, (tile, d), 0) + t * tile < p_ref[r]
            first = kc[r, 0:16, :].astype(f32)[0:1]
            kc[r, at, :] = jnp.where(there, kc[r, at, :].astype(f32), first).astype(bf)
            vext[r, at, :d] = jnp.where(there, vc[r, at, :].astype(f32), 0.0).astype(bf)
            vext[r, at, d:] = jnp.where(there, 1.0, 0.0).astype(bf)
            return 0

        lax.fori_loop(0, old // tile, tidy, 0)
    vn_ext[:, :, d:] = jnp.ones((n_req, vn_ext.shape[1], d), bf)
    for c in loads:
        c.wait()

    def tick(s):
        @pl.when(s < nz)
        def _():
            for h in range(CHUNKS):
                for way in range(2):
                    ring_copy(s - 1, way, h).wait_recv()

                    @pl.when(s < nz - 1)
                    def _():
                        ring_copy(s, way, h).start()

            for way in range(2):
                pair_copy(s, way).start()

                @pl.when(s <= reach[way])
                def _():
                    a_copy(s - 1, way).wait_recv()

                    @pl.when(s < reach[way])
                    def _():
                        a_copy(s, way).start()

                    for k in range(1, n_dp):
                        b_copy(s, way, k).start()

    scale2 = (d ** -0.5) * math.log2(math.e)
    block = old // KEY_BLOCKS
    nt = (((1,), (1,)), ((), ()))

    def flash(s, m_prev, acc, vals):
        m_new = jnp.maximum(m_prev, jnp.max(s, axis=1, keepdims=True))
        a = jnp.exp2((m_prev - m_new) * scale2)
        p = jnp.exp2((s - m_new[:, :1]) * scale2).astype(bf)
        return m_new, acc * jnp.concatenate([a, a], axis=1) + jnp.dot(p, vals, preferred_element_type=f32)

    tick(1)

    def places(k):
        for t in range(2):
            for way in range(2):
                for other in range(2):
                    off = pl.multiple_of((away(2 * k + t, way) * 2 + (core if other == 0 else 1 - core)) * n_rows, n_rows)
                    yield t, way, other, off

    def project(k):
        for t in range(2):
            for way in range(2):
                pair_copy(2 * k + t, way).wait_recv()
        lhs = rows[pl.ds(2 * k, 2)].reshape(8 * n_rows, width)
        total = jnp.dot(lhs, w[...], preferred_element_type=f32)
        got = [(total[:, i * d:(i + 1) * d] + b[...].astype(f32).reshape(1, d)).astype(bf) for i, b in enumerate((bq_ref, bk_ref, bv_ref))]
        sign = jnp.where(lax.broadcasted_iota(jnp.int32, (n_rows, d), 1) < d // 2, -1.0, 1.0)

        for t, way, other, off in places(k):
            at = pl.ds(off, n_rows)
            spot = (lax.broadcasted_iota(jnp.int32, (n_rows, d), 0) + (p_ref[way] + off)).astype(f32)
            angle = spot * f_ref[...]
            cos_t = jnp.cos(angle)
            sin_t = jnp.sin(angle) * sign
            i = ((t * 2 + way) * 2 + other) * n_rows
            turned = []
            for part in got[:2]:
                part = part[i:i + n_rows].astype(f32)
                turned.append((part * cos_t + pltpu.roll(part, d // 2, 1) * sin_t).astype(bf))
            q_abs[way, at, :] = turned[0]
            q_now[way, pl.ds(t * two + other * n_rows, n_rows), :] = turned[0]
            kn_ref[way, at, :] = turned[1]
            vn_ref[way, at, :] = got[2][i:i + n_rows]
            vn_ext[way, at, :d] = got[2][i:i + n_rows]

    def attend_old(k, ticks):
        m_now[...] = jnp.full_like(m_now, NEG)
        acc_now[...] = jnp.zeros_like(acc_now)

        def keys(j, _):
            at = pl.ds(pl.multiple_of(j * block, block), block)
            for u in range(2):
                for way in range(2):
                    sl = pl.ds(u * two, two)
                    s = lax.dot_general(q_now[way, sl, :], kc[way, at, :], nt, preferred_element_type=f32)
                    m_now[way, sl, :], acc_now[way, sl, :] = flash(s, m_now[way, sl, :], acc_now[way, sl, :], vext[way, at, :])

            if ticks:
                @pl.when(j == KEY_BLOCKS // 2 - 1)
                def _():
                    tick(2 * k + 2)

                @pl.when(j == KEY_BLOCKS - 1)
                def _():
                    tick(2 * k + 3)
            return 0

        lax.fori_loop(0, KEY_BLOCKS, keys, 0)
        for t, way, other, off in places(k):
            at = pl.ds(off, n_rows)
            here = pl.ds(t * two + other * n_rows, n_rows)
            m_abs[way, at, :] = m_now[way, here, :]
            acc_abs[way, at, :] = acc_now[way, here, :]

    def two_steps(k, _):
        project(k)
        attend_old(k, True)
        return 0

    last = nz // 2 - 1
    lax.fori_loop(0, last, two_steps, 0)
    project(last)

    pieces = [(s, way) for s in range(1, nz // 2 + 1) for way in range(2) if s <= reach[way]]
    for s, way in pieces:
        for k in range(1, n_dp):
            b_copy(s, way, k, lax.rem(group + n_dp - k, n_dp)).wait_recv()
        c_copy(s, way).start()

    mine = pl.ds(pl.multiple_of(me * d, d), d)

    def o_copy(s, way, to):
        home = away(s, way)
        off = pl.multiple_of(home * two + to * n_rows, n_rows)
        return remote(o_v.at[way, pl.ds(off, n_rows), :], o_all.at[way, :, mine], o_send.at[s, way, to], o_recv.at[s, way, core], home * 2 + to)

    def finish(i, _):
        for way in range(2):
            home = away(i, way)
            at = pl.ds(pl.multiple_of(home * two, two), two)
            s = lax.dot_general(q_abs[way, at, :], kn_ref[way], nt, preferred_element_type=f32)
            rid = lax.broadcasted_iota(jnp.int32, (two, 1), 0) + home * two
            s = jnp.where(lax.broadcasted_iota(jnp.int32, s.shape, 1) <= jnp.minimum(rid, c_ref[way] - 1), s, NEG)
            m_prev = jnp.where(jnp.full((two, d), p_ref[way], jnp.int32) > 0, m_abs[way, at, :], NEG)
            _, acc = flash(s, m_prev, acc_abs[way, at, :], vn_ext[way])
            o_v[way, at, :] = (acc[:, :d] / acc[:, d:]).astype(bf)
        for way in range(2):
            for to in range(2):
                @pl.when((i > 0) | (core != to))
                def _():
                    o_copy(i, way, to).start()

                @pl.when((i == 0) & (core == to))
                def _():
                    o_all[way, :, mine] = o_v[way, pl.ds(pl.multiple_of(chip * two + to * n_rows, n_rows), n_rows), :]
        return 0

    lax.fori_loop(0, 2 * last, finish, 0)
    attend_old(last, False)
    lax.fori_loop(2 * last, nz, finish, 0)

    def o_wait(i, _):
        for way in range(2):
            for to in range(2):
                @pl.when((i > 0) | (core != to))
                def _():
                    source = away(i, 1 - way) * 2 + to
                    spot = pl.ds(pl.multiple_of(source * d, d), d)
                    remote(o_v.at[way, pl.ds(0, n_rows), :], o_all.at[way, :, spot], o_send.at[i, way, to], o_recv.at[i, way, to], pair).wait_recv()
                    o_copy(i, way, to).wait_send()
        return 0

    lax.fori_loop(0, nz, o_wait, 0)

    own_store.wait()
    c_copy(0, 0, wo).wait_send()
    c_wait(0, 0)
    for way in range(2):
        a_copy(0, way, own_share).wait_send()
    for s, way in pieces:
        c_wait(s, way)
        c_copy(s, way).wait_send()
        for k in range(1, n_dp):
            b_copy(s, way, k).wait_send()
        if s < reach[way]:
            a_copy(s, way).wait_send()
    for s in range(nz):
        for way in range(2):
            pair_copy(s, way).wait_send()
            if s < nz - 1:
                for h in range(CHUNKS):
                    ring_copy(s, way, h).wait_send()


def front(n_tp, n_dp, x, gain, prefix, valid, freq, b_q, b_k, b_v, w_q, w_k, w_v, w_o, k_cache, v_cache):
    n_req, n_rows, width = x.shape
    d = w_q.shape[1]
    nz = n_tp // 2
    n_tok = n_rows * n_tp
    slots = k_cache.shape[1]
    old = slots - n_tok
    bf, f32 = jnp.bfloat16, jnp.float32
    any_spec = pl.BlockSpec(memory_space=pl.ANY)
    sm = pl.BlockSpec(memory_space=pltpu.SMEM)
    vm = pl.BlockSpec(memory_space=pltpu.VMEM)
    dma = pltpu.SemaphoreType.DMA
    made = jax.ShapeDtypeStruct((n_req, n_tok, d), bf)
    return pl.pallas_call(
        functools.partial(front_kernel, n_tp, n_dp),
        out_shape=[jax.ShapeDtypeStruct(x.shape, bf), made, made, jax.ShapeDtypeStruct((n_tp * d, width), bf)],
        in_specs=[sm, sm, vm, vm, vm, vm, vm, vm] + [any_spec] * 6,
        out_specs=[vm, vm, vm, any_spec],
        scratch_shapes=[
            pltpu.VMEM((width, 3 * d), bf),
            pltpu.VMEM((nz, 2, 2, n_rows, width), bf),
            pltpu.VMEM(w_o.shape, bf),
            pltpu.VMEM((n_req, old, d), bf),
            pltpu.VMEM((n_req, old, d), bf),
            pltpu.VMEM((n_req, old, 2 * d), bf),
            pltpu.VMEM((n_req, n_tok, d), bf),
            pltpu.VMEM((n_req, n_tok, 2 * d), bf),
            pltpu.VMEM((n_req, n_tok, d), f32),
            pltpu.VMEM((n_req, n_tok, 2 * d), f32),
            pltpu.VMEM((n_req, 4 * n_rows, d), bf),
            pltpu.VMEM((n_req, 4 * n_rows, d), f32),
            pltpu.VMEM((n_req, 4 * n_rows, 2 * d), f32),
            pltpu.VMEM((n_req, n_tok, d), bf),
            dma((4,)), dma((2,)), dma((nz, 2, CHUNKS)), dma((nz, 2, CHUNKS)), dma((nz, 2)), dma((nz, 2)),
            dma((nz, 2)), dma((nz, 2)), dma((nz, 2, n_dp)), dma((nz, 2, n_dp)), dma((nz, 2)), dma((nz, 2)),
            dma((nz, 2, 2)), dma((nz, 2, 2)),
        ],
        compiler_params=pltpu.CompilerParams(vmem_limit_bytes=62 * 2**20, collective_id=2, has_side_effects=True),
        cost_estimate=pl.CostEstimate(flops=8 * n_req * n_tok * slots * d, bytes_accessed=20 * 2**20, transcendentals=n_req * n_tok * slots),
        name="front",
    )(prefix, valid, x, gain, freq, b_q, b_k, b_v, w_q, w_k, w_v, w_o, k_cache, v_cache)


def merge_kernel(p_ref, c_ref, kn_ref, vn_ref, kc_hbm, vc_hbm, ko_hbm, vo_hbm, cache, shift, sems):
    n_req, n_tok, d = kn_ref.shape
    slots = ko_hbm.shape[1]
    win = n_tok + 16
    news, olds, outs = (kn_ref, vn_ref), (kc_hbm, vc_hbm), (ko_hbm, vo_hbm)
    pairs = [(r, i) for r in range(n_req) for i in range(2)]
    moves_in = [pltpu.make_async_copy(olds[i].at[r], cache.at[r, i], sems.at[0, r, i]) for r, i in pairs]
    moves_out = [pltpu.make_async_copy(cache.at[r, i], outs[i].at[r], sems.at[1, r, i]) for r, i in pairs]
    for c in moves_in:
        c.start()
    for n, (r, i) in enumerate(pairs):
        start = pl.multiple_of(jnp.minimum((p_ref[r] // 16) * 16, slots - win), 16)
        off = p_ref[r] - start
        at = lax.broadcasted_iota(jnp.int32, (win, d), 0) - off
        fresh = (at >= 0) & (at < c_ref[r])
        shift[pl.ds(16, n_tok), :] = news[i][r].astype(jnp.float32)
        moved = shift[pl.ds(16 - off, win), :]
        moves_in[n].wait()
        part = pl.ds(start, win)
        cache[r, i, part, :] = jnp.where(fresh, moved, cache[r, i, part, :].astype(jnp.float32)).astype(cache.dtype)
        moves_out[n].start()
    for c in moves_out:
        c.wait()


def merge(prefix, valid, k_new, v_new, k_cache, v_cache):
    n_req, n_tok, d = k_new.shape
    slots = k_cache.shape[1]
    any_spec = pl.BlockSpec(memory_space=pl.ANY)
    sm = pl.BlockSpec(memory_space=pltpu.SMEM)
    vm = pl.BlockSpec(memory_space=pltpu.VMEM)
    same = jax.ShapeDtypeStruct(k_cache.shape, k_cache.dtype)
    return pl.pallas_call(
        merge_kernel,
        out_shape=[same, same],
        in_specs=[sm, sm, vm, vm, any_spec, any_spec],
        out_specs=[any_spec, any_spec],
        scratch_shapes=[
            pltpu.VMEM((n_req, 2, slots, d), k_cache.dtype),
            pltpu.VMEM((n_tok + 32, d), jnp.float32),
            pltpu.SemaphoreType.DMA((2, n_req, 2)),
        ],
        compiler_params=pltpu.CompilerParams(vmem_limit_bytes=62 * 2**20),
        cost_estimate=pl.CostEstimate(flops=10**6, bytes_accessed=16 * 2**20, transcendentals=0),
        name="merge",
    )(prefix, valid, k_new, v_new, k_cache, v_cache)


def solution(mesh):
    n_tp = mesh.shape["tp"]
    row_spec = P("dp", "tp", None)
    cache_spec = P("dp", None, "tp", None)
    req_spec = P("dp")
    rep_spec = P(None)
    col_spec = P(None, "tp")
    bias_spec = P("tp")
    down_spec = P("tp", None)

    def layer(x_rows, k_cache, v_cache, prefix, valid, g_attn, w_q, b_q, w_k, b_k, w_v, b_v, w_o, g_mlp, w_gate, w_up, w_down):
        n_req, head_dim = x_rows.shape[0], k_cache.shape[-1]
        half = np.arange(head_dim // 2, dtype=np.float32)
        freq = np.float32(ROPE_THETA) ** (-(half * np.float32(2.0)) / np.float32(head_dim))
        freq = jnp.asarray(np.concatenate([freq, freq])[None], jnp.float32)
        flat = (n_req, -1, head_dim)
        k_flat, v_flat = k_cache.reshape(flat), v_cache.reshape(flat)
        o, k_new, v_new, w_o_full = front(n_tp, mesh.shape["dp"], x_rows, g_attn, prefix, valid, freq, b_q, b_k, b_v, w_q, w_k, w_v, w_o, k_flat, v_flat)
        k_out, v_out = merge(prefix, valid, k_new, v_new, k_flat, v_flat)
        out = tail(n_tp, o, x_rows, g_mlp, w_o_full, w_gate.T, w_up.T, w_down)
        return out, k_out.reshape(k_cache.shape), v_out.reshape(v_cache.shape)

    in_specs = (row_spec, cache_spec, cache_spec, req_spec, req_spec, rep_spec, col_spec, bias_spec, col_spec, bias_spec, col_spec, bias_spec, down_spec, rep_spec, col_spec, col_spec, down_spec)
    return jax.shard_map(layer, mesh=mesh, in_specs=in_specs, out_specs=(row_spec, cache_spec, cache_spec), check_vma=False)
```

```python
import functools
import math

import jax
import jax.numpy as jnp
import numpy as np
from jax import lax
from jax.experimental import pallas as pl
from jax.experimental.pallas import tpu as pltpu
from jax.sharding import PartitionSpec as P

ROPE_THETA = 1.0e6
NORM_EPS = 1.0e-6


CHUNKS = 1
WO_BITES = 4
MESH = pl.DeviceIdType.MESH


def remote(src, dst, send, recv, target):
    return pltpu.make_async_remote_copy(src_ref=src, dst_ref=dst, send_sem=send, recv_sem=recv, device_id={"tp": target}, device_id_type=MESH)


def tail_kernel(n_tp, o_all, x_ref, g_ref, wo_hbm, wg_hbm, wu_hbm, wd_hbm, out_ref,
                wo, wg, wu, wd, x1, rows, sums_in, sums_out, part_in, part_out, kept,
                load_sem, bite_sem, ring_send, ring_recv, pair_send, pair_recv, sum_send, sum_recv, part_send, part_recv):
    nz = n_tp // 2
    me = lax.axis_index("tp")
    core = lax.rem(me, 2)
    chip = me // 2
    up = lax.rem(chip + 1, nz) * 2 + core
    down = lax.rem(chip + nz - 1, nz) * 2 + core
    pair = chip * 2 + 1 - core
    towards = (up, down)
    n_req, n_rows, width = x_ref.shape

    loads = [pltpu.make_async_copy(s, t, load_sem.at[i]) for i, (s, t) in enumerate(((wg_hbm, wg), (wu_hbm, wu), (wd_hbm, wd)))]
    bite = wo.shape[0] // WO_BITES
    bites = [pltpu.make_async_copy(wo_hbm.at[pl.ds(i * bite, bite)], wo.at[pl.ds(i * bite, bite)], bite_sem.at[i]) for i in range(WO_BITES)]
    for c in bites:
        c.start()

    barrier = pltpu.get_barrier_semaphore()
    for there in (up, down, pair):
        pl.semaphore_signal(barrier, inc=1, device_id={"tp": there}, device_id_type=MESH)

    heads = o_all[...].reshape(n_req * n_rows, width)
    mixed = None
    for i in range(WO_BITES):
        bites[i].wait()
        if i == WO_BITES - 1:
            for c in loads:
                c.start()
        at = slice(i * bite, (i + 1) * bite)
        piece = jnp.dot(heads[:, at], wo[at, :], preferred_element_type=jnp.float32)
        mixed = piece if mixed is None else mixed + piece
    mixed = mixed.astype(jnp.bfloat16)
    resid = (x_ref[...].reshape(n_req * n_rows, width).astype(jnp.float32) + mixed.astype(jnp.float32)).astype(jnp.bfloat16)
    x1[...] = resid.reshape(x1.shape)
    wide = resid.astype(jnp.float32)
    inv = lax.rsqrt(jnp.mean(wide * wide, axis=-1, keepdims=True) + NORM_EPS)
    normed = (wide * inv * g_ref[...].astype(jnp.float32).reshape(1, width)).astype(jnp.bfloat16)
    pl.semaphore_wait(barrier, 3)
    rows[0, :, 0] = normed.reshape(n_req, n_rows, width)

    for c in loads:
        c.wait()

    span = n_rows // CHUNKS

    def ring_copy(s, way, h):
        part = pl.ds(h * span, span)
        return remote(rows.at[s, way, 0, part], rows.at[s + 1, way, 0, part], ring_send.at[s, way, h], ring_recv.at[s + 1, way, h], towards[way])

    def pair_copy(s, way):
        return remote(rows.at[s, way, 0], rows.at[s, way, 1], pair_send.at[s, way], pair_recv.at[s, way], pair)

    def part_copy(s):
        return remote(part_out.at[s], part_in.at[s], part_send.at[s], part_recv.at[s], pair)

    def sum_copy(s, way, h):
        part = pl.ds(h * span, span)
        return remote(sums_out.at[s, way, part], sums_in.at[s + 1, way, part], sum_send.at[s, way, h], sum_recv.at[s + 1, way, h], towards[way])

    def step(s, _):
        for h in range(CHUNKS):
            for way in range(2):
                @pl.when(s > 0)
                def _():
                    ring_copy(s - 1, way, h).wait_recv()

                @pl.when(s < nz - 1)
                def _():
                    ring_copy(s, way, h).start()

        for way in range(2):
            pair_copy(s, way).start()
        for way in range(2):
            pair_copy(s, way).wait_recv()
        lhs = rows[s].reshape(4 * n_rows, width)
        gate = lax.dot_general(lhs, wg[...], (((1,), (1,)), ((), ())), preferred_element_type=jnp.float32)
        lift = lax.dot_general(lhs, wu[...], (((1,), (1,)), ((), ())), preferred_element_type=jnp.float32)
        act = (jax.nn.silu(gate) * lift).astype(jnp.bfloat16)
        part = jnp.dot(act, wd[...], preferred_element_type=jnp.float32).reshape(2, 2, n_rows, width)
        part_out[s] = part[:, 1].astype(jnp.bfloat16)
        part_copy(s).start()
        kept[jnp.minimum(s, 1)] = part[:, 0]

        @pl.when(s > 0)
        def _():
            part_copy(s).wait_recv()
            for h in range(CHUNKS):
                part = pl.ds(h * span, span)
                for way in range(2):
                    @pl.when(s > 1)
                    def _():
                        sum_copy(s - 1, way, h).wait_recv()
                        sums_out[s, way, part] = (kept[1, way, part] + part_in[s, way, part].astype(jnp.float32) + sums_in[s, way, part].astype(jnp.float32)).astype(jnp.bfloat16)

                    @pl.when(s == 1)
                    def _():
                        sums_out[s, way, part] = (kept[1, way, part] + part_in[s, way, part].astype(jnp.float32)).astype(jnp.bfloat16)

                    sum_copy(s, way, h).start()
        return 0

    lax.fori_loop(0, nz, step, 0)

    part_copy(0).wait_recv()
    for h in range(CHUNKS):
        part = pl.ds(h * span, span)
        for way in range(2):
            sum_copy(nz - 1, way, h).wait_recv()
            total = kept[0, way, part] + part_in[0, way, part].astype(jnp.float32) + sums_in[nz, way, part].astype(jnp.float32)
            out_ref[way, part] = (x1[way, part].astype(jnp.float32) + total.astype(jnp.bfloat16).astype(jnp.float32)).astype(jnp.bfloat16)

    for s in range(nz):
        part_copy(s).wait_send()
        for way in range(2):
            pair_copy(s, way).wait_send()
            if s < nz - 1:
                for h in range(CHUNKS):
                    ring_copy(s, way, h).wait_send()
            if s > 0:
                for h in range(CHUNKS):
                    sum_copy(s, way, h).wait_send()


def tail(n_tp, o, x, gain, w_o, w_gate, w_up, w_down):
    n_req, n_rows, width = x.shape
    ffn = w_gate.shape[0]
    nz = n_tp // 2
    bf = jnp.bfloat16
    any_spec = pl.BlockSpec(memory_space=pl.ANY)
    vm = pl.BlockSpec(memory_space=pltpu.VMEM)
    dma = pltpu.SemaphoreType.DMA
    return pl.pallas_call(
        functools.partial(tail_kernel, n_tp),
        out_shape=jax.ShapeDtypeStruct(x.shape, x.dtype),
        in_specs=[vm, vm, vm, any_spec, any_spec, any_spec, any_spec],
        out_specs=vm,
        scratch_shapes=[
            pltpu.VMEM(w_o.shape, bf),
            pltpu.VMEM(w_gate.shape, bf),
            pltpu.VMEM(w_up.shape, bf),
            pltpu.VMEM(w_down.shape, bf),
            pltpu.VMEM((n_req, n_rows, width), bf),
            pltpu.VMEM((nz, 2, 2, n_rows, width), bf),
            pltpu.VMEM((nz + 1, 2, n_rows, width), bf),
            pltpu.VMEM((nz, 2, n_rows, width), bf),
            pltpu.VMEM((nz, 2, n_rows, width), bf),
            pltpu.VMEM((nz, 2, n_rows, width), bf),
            pltpu.VMEM((2, 2, n_rows, width), jnp.float32),
            dma((3,)), dma((WO_BITES,)),
            dma((nz, 2, CHUNKS)), dma((nz, 2, CHUNKS)), dma((nz, 2)), dma((nz, 2)),
            dma((nz, 2, CHUNKS)), dma((nz + 1, 2, CHUNKS)), dma((nz,)), dma((nz,)),
        ],
        compiler_params=pltpu.CompilerParams(vmem_limit_bytes=62 * 2**20, collective_id=1, has_side_effects=True),
        cost_estimate=pl.CostEstimate(flops=6 * n_tp * n_req * n_rows * width * ffn, bytes_accessed=20 * 2**20, transcendentals=0),
        name="tail",
    )(o, x, gain, w_o, w_gate, w_up, w_down)


NEG = -1.0e30
KEY_BLOCKS = 4
STREAMS = 2


def front_kernel(n_tp, n_dp, p_ref, c_ref, x_ref, g_ref, f_ref, bq_ref, bk_ref, bv_ref, wq_hbm, wk_hbm, wv_hbm, wo_hbm, kc_hbm, vc_hbm,
                 o_all, kn_ref, vn_ref, all_hbm,
                 w, rows, wo, cos_v, sin_v, kc, vc, vext, q_abs, vn_ext, m_abs, acc_abs, q_now, m_now, acc_now, o_v,
                 load_sem, cache_sem, ring_send, ring_recv, pair_send, pair_recv, a_send, a_recv, b_send, b_recv, c_send, c_recv, o_send, o_recv):
    nz = n_tp // 2
    me = lax.axis_index("tp")
    core = lax.rem(me, 2)
    chip = me // 2
    group = lax.axis_index("dp")
    up = lax.rem(chip + 1, nz) * 2 + core
    down = lax.rem(chip + nz - 1, nz) * 2 + core
    pair = chip * 2 + 1 - core
    towards = (up, down)
    n_req, n_rows, width = x_ref.shape
    d = q_abs.shape[-1]
    two = 2 * n_rows
    old = vext.shape[1]
    bf, f32 = jnp.bfloat16, jnp.float32

    own_load = pltpu.make_async_copy(wo_hbm, wo, load_sem.at[3])
    own_load.start()
    loads = [pltpu.make_async_copy(s, w.at[:, pl.ds(i * d, d)], load_sem.at[i]) for i, s in enumerate((wq_hbm, wk_hbm, wv_hbm))]
    for c in loads:
        c.start()
    cache_in = [pltpu.make_async_copy(s.at[:, pl.ds(0, old)], t, cache_sem.at[i]) for i, (s, t) in enumerate(((kc_hbm, kc), (vc_hbm, vc)))]
    for c in cache_in:
        c.start()

    barrier = pltpu.get_barrier_semaphore()
    for k in range(1, n_tp):
        pl.semaphore_signal(barrier, inc=1, device_id={"tp": lax.rem(me + k, n_tp)}, device_id_type=MESH)
    for k in range(1, n_dp):
        pl.semaphore_signal(barrier, inc=1, device_id={"dp": lax.rem(group + k, n_dp)}, device_id_type=MESH)

    wide = x_ref[...].astype(f32)
    inv = lax.rsqrt(jnp.mean(wide * wide, axis=-1, keepdims=True) + NORM_EPS)
    rows[0, :, 0] = (wide * inv * g_ref[...].astype(f32).reshape(1, width)).astype(bf)
    pl.semaphore_wait(barrier, n_tp + n_dp - 2)

    span = n_rows // STREAMS

    def ring_copy(s, way, h):
        part = pl.ds(pl.multiple_of(h * span, span), span)
        return remote(rows.at[s, way, 0, part], rows.at[s + 1, way, 0, part], ring_send.at[s, way, h], ring_recv.at[s + 1, way, h], towards[way])

    def pair_copy(s, way):
        return remote(rows.at[s, way, 0], rows.at[s, way, 1], pair_send.at[s, way], pair_recv.at[s, way], pair)

    n_own = wo.shape[0]
    share = n_own // n_dp
    reach = (nz // 2, (nz - 1) // 2)

    def away(s, way):
        return lax.rem(chip + (nz - s if way == 0 else s), nz)

    def home_rows(s, way, part, count):
        return pl.ds(pl.multiple_of((away(s, way) * 2 + core) * n_own + part * share, 8), count)

    def a_copy(s, way, src=None):
        at = home_rows(s, way, group, share)
        return remote(all_hbm.at[at] if src is None else src, all_hbm.at[at], a_send.at[s, way], a_recv.at[s + 1, way], towards[way])

    def b_copy(s, way, k, owner=None):
        at = home_rows(s, way, group if owner is None else owner, share)
        return pltpu.make_async_remote_copy(src_ref=all_hbm.at[at], dst_ref=all_hbm.at[at], send_sem=b_send.at[s, way, k], recv_sem=b_recv.at[s, way, k],
                                            device_id={"dp": lax.rem(group + k, n_dp)}, device_id_type=MESH)

    def c_copy(s, way, src=None):
        at = home_rows(s, way, 0, n_own)
        return remote(all_hbm.at[at] if src is None else src, all_hbm.at[at], c_send.at[s, way], c_recv.at[s, way], pair)

    def c_wait(s, way):
        at = pl.ds(pl.multiple_of((away(s, way) * 2 + 1 - core) * n_own, 8), n_own)
        remote(all_hbm.at[at], all_hbm.at[at], c_send.at[s, way], c_recv.at[s, way], pair).wait_recv()

    for h in range(STREAMS):
        for way in range(2):
            ring_copy(0, way, h).start()
    for way in range(2):
        pair_copy(0, way).start()
    own_load.wait()
    own_share = wo.at[pl.ds(pl.multiple_of(group * share, 8), share)]
    own_store = pltpu.make_async_copy(wo, all_hbm.at[home_rows(0, 0, 0, n_own)], load_sem.at[3])
    for way in range(2):
        a_copy(0, way, own_share).start()
    own_store.start()
    c_copy(0, 0, wo).start()

    for c in cache_in:
        c.wait()
    tile = 1024
    for r in range(n_req):
        def tidy(t, _):
            at = pl.ds(pl.multiple_of(t * tile, tile), tile)
            there = lax.broadcasted_iota(jnp.int32, (tile, d), 0) + t * tile < p_ref[r]
            first = kc[r, 0:16, :].astype(f32)[0:1]
            kc[r, at, :] = jnp.where(there, kc[r, at, :].astype(f32), first).astype(bf)
            vext[r, at, :d] = jnp.where(there, vc[r, at, :].astype(f32), 0.0).astype(bf)
            vext[r, at, d:] = jnp.where(there, 1.0, 0.0).astype(bf)
            return 0

        lax.fori_loop(0, old // tile, tidy, 0)
    turn = 128
    sign = jnp.where(lax.broadcasted_iota(jnp.int32, (turn, d), 1) < d // 2, -1.0, 1.0)
    for r in range(n_req):
        def angles(t, _):
            spot = (lax.broadcasted_iota(jnp.int32, (turn, d), 0) + (p_ref[r] + t * turn)).astype(f32)
            angle = spot * f_ref[...]
            at = pl.ds(pl.multiple_of(t * turn, turn), turn)
            cos_v[r, at, :] = jnp.cos(angle)
            sin_v[r, at, :] = jnp.sin(angle) * sign
            return 0

        lax.fori_loop(0, cos_v.shape[1] // turn, angles, 0)
    vn_ext[:, :, d:] = jnp.ones((n_req, vn_ext.shape[1], d), bf)
    for c in loads:
        c.wait()

    def pass_on(s, h):
        @pl.when(s < nz)
        def _():
            for way in range(2):
                ring_copy(s - 1, way, h).wait_recv()

                @pl.when(s < nz - 1)
                def _():
                    ring_copy(s, way, h).start()

    def landed(s):
        @pl.when(s < nz)
        def _():
            for way in range(2):
                pair_copy(s, way).start()

                @pl.when(s <= reach[way])
                def _():
                    a_copy(s - 1, way).wait_recv()

                    @pl.when(s < reach[way])
                    def _():
                        a_copy(s, way).start()

                    for k in range(1, n_dp):
                        b_copy(s, way, k).start()

    scale2 = (d ** -0.5) * math.log2(math.e)
    block = old // KEY_BLOCKS
    nt = (((1,), (1,)), ((), ()))

    def flash(s, m_prev, acc, vals):
        m_new = jnp.maximum(m_prev, jnp.max(s, axis=1, keepdims=True))
        a = jnp.exp2((m_prev - m_new) * scale2)
        p = jnp.exp2((s - m_new[:, :1]) * scale2).astype(bf)
        return m_new, acc * jnp.concatenate([a, a], axis=1) + jnp.dot(p, vals, preferred_element_type=f32)

    for h in range(STREAMS):
        pass_on(1, h)
    landed(1)

    def places(k):
        for t in range(2):
            for way in range(2):
                for other in range(2):
                    off = pl.multiple_of((away(2 * k + t, way) * 2 + (core if other == 0 else 1 - core)) * n_rows, n_rows)
                    yield t, way, other, off

    def project(k):
        for t in range(2):
            for way in range(2):
                pair_copy(2 * k + t, way).wait_recv()
        lhs = rows[pl.ds(2 * k, 2)].reshape(8 * n_rows, width)
        total = jnp.dot(lhs, w[...], preferred_element_type=f32)
        got = [(total[:, i * d:(i + 1) * d] + b[...].astype(f32).reshape(1, d)).astype(bf) for i, b in enumerate((bq_ref, bk_ref, bv_ref))]

        for t, way, other, off in places(k):
            at = pl.ds(off, n_rows)
            cos_t, sin_t = cos_v[way, at, :], sin_v[way, at, :]
            i = ((t * 2 + way) * 2 + other) * n_rows
            turned = []
            for part in got[:2]:
                part = part[i:i + n_rows].astype(f32)
                turned.append((part * cos_t + pltpu.roll(part, d // 2, 1) * sin_t).astype(bf))
            q_abs[way, at, :] = turned[0]
            q_now[way, pl.ds(t * two + other * n_rows, n_rows), :] = turned[0]
            kn_ref[way, at, :] = turned[1]
            vn_ref[way, at, :] = got[2][i:i + n_rows]
            vn_ext[way, at, :d] = got[2][i:i + n_rows]

    def attend_old(k, ticks):
        m_now[...] = jnp.full_like(m_now, NEG)
        acc_now[...] = jnp.zeros_like(acc_now)

        def keys(j, _):
            at = pl.ds(pl.multiple_of(j * block, block), block)
            for u in range(2):
                for way in range(2):
                    sl = pl.ds(u * two, two)
                    s = lax.dot_general(q_now[way, sl, :], kc[way, at, :], nt, preferred_element_type=f32)
                    m_now[way, sl, :], acc_now[way, sl, :] = flash(s, m_now[way, sl, :], acc_now[way, sl, :], vext[way, at, :])

            if ticks:
                for n in range(2 * STREAMS // KEY_BLOCKS):
                    event = j * (2 * STREAMS // KEY_BLOCKS) + n
                    step = 2 * k + 2 + event // STREAMS
                    pass_on(step, lax.rem(event, STREAMS))

                    @pl.when(lax.rem(event, STREAMS) == STREAMS - 1)
                    def _():
                        landed(step)
            return 0

        lax.fori_loop(0, KEY_BLOCKS, keys, 0)
        for t, way, other, off in places(k):
            at = pl.ds(off, n_rows)
            here = pl.ds(t * two + other * n_rows, n_rows)
            m_abs[way, at, :] = m_now[way, here, :]
            acc_abs[way, at, :] = acc_now[way, here, :]

    def two_steps(k, _):
        project(k)
        attend_old(k, True)
        return 0

    last = nz // 2 - 1
    lax.fori_loop(0, last, two_steps, 0)
    project(last)

    pieces = [(s, way) for s in range(1, nz // 2 + 1) for way in range(2) if s <= reach[way]]
    for s, way in pieces:
        for k in range(1, n_dp):
            b_copy(s, way, k, lax.rem(group + n_dp - k, n_dp)).wait_recv()
        c_copy(s, way).start()

    mine = pl.ds(pl.multiple_of(me * d, d), d)

    def o_copy(s, way, to):
        home = away(s, way)
        off = pl.multiple_of(home * two + to * n_rows, n_rows)
        return remote(o_v.at[way, pl.ds(off, n_rows), :], o_all.at[way, :, mine], o_send.at[s, way, to], o_recv.at[s, way, core], home * 2 + to)

    def finish(i, _):
        for way in range(2):
            home = away(i, way)
            at = pl.ds(pl.multiple_of(home * two, two), two)
            s = lax.dot_general(q_abs[way, at, :], kn_ref[way], nt, preferred_element_type=f32)
            rid = lax.broadcasted_iota(jnp.int32, (two, 1), 0) + home * two
            s = jnp.where(lax.broadcasted_iota(jnp.int32, s.shape, 1) <= jnp.minimum(rid, c_ref[way] - 1), s, NEG)
            m_prev = jnp.where(jnp.full((two, d), p_ref[way], jnp.int32) > 0, m_abs[way, at, :], NEG)
            _, acc = flash(s, m_prev, acc_abs[way, at, :], vn_ext[way])
            o_v[way, at, :] = (acc[:, :d] / acc[:, d:]).astype(bf)
        for way in range(2):
            for to in range(2):
                @pl.when((i > 0) | (core != to))
                def _():
                    o_copy(i, way, to).start()

                @pl.when((i == 0) & (core == to))
                def _():
                    o_all[way, :, mine] = o_v[way, pl.ds(pl.multiple_of(chip * two + to * n_rows, n_rows), n_rows), :]
        return 0

    lax.fori_loop(0, 2 * last, finish, 0)
    attend_old(last, False)
    lax.fori_loop(2 * last, nz, finish, 0)

    def o_wait(i, _):
        for way in range(2):
            for to in range(2):
                @pl.when((i > 0) | (core != to))
                def _():
                    source = away(i, 1 - way) * 2 + to
                    spot = pl.ds(pl.multiple_of(source * d, d), d)
                    remote(o_v.at[way, pl.ds(0, n_rows), :], o_all.at[way, :, spot], o_send.at[i, way, to], o_recv.at[i, way, to], pair).wait_recv()
                    o_copy(i, way, to).wait_send()
        return 0

    lax.fori_loop(0, nz, o_wait, 0)

    own_store.wait()
    c_copy(0, 0, wo).wait_send()
    c_wait(0, 0)
    for way in range(2):
        a_copy(0, way, own_share).wait_send()
    for s, way in pieces:
        c_wait(s, way)
        c_copy(s, way).wait_send()
        for k in range(1, n_dp):
            b_copy(s, way, k).wait_send()
        if s < reach[way]:
            a_copy(s, way).wait_send()
    for s in range(nz):
        for way in range(2):
            pair_copy(s, way).wait_send()
            if s < nz - 1:
                for h in range(STREAMS):
                    ring_copy(s, way, h).wait_send()


def front(n_tp, n_dp, x, gain, prefix, valid, freq, b_q, b_k, b_v, w_q, w_k, w_v, w_o, k_cache, v_cache):
    n_req, n_rows, width = x.shape
    d = w_q.shape[1]
    nz = n_tp // 2
    n_tok = n_rows * n_tp
    slots = k_cache.shape[1]
    old = slots - n_tok
    bf, f32 = jnp.bfloat16, jnp.float32
    any_spec = pl.BlockSpec(memory_space=pl.ANY)
    sm = pl.BlockSpec(memory_space=pltpu.SMEM)
    vm = pl.BlockSpec(memory_space=pltpu.VMEM)
    dma = pltpu.SemaphoreType.DMA
    made = jax.ShapeDtypeStruct((n_req, n_tok, d), bf)
    return pl.pallas_call(
        functools.partial(front_kernel, n_tp, n_dp),
        out_shape=[jax.ShapeDtypeStruct(x.shape, bf), made, made, jax.ShapeDtypeStruct((n_tp * d, width), bf)],
        in_specs=[sm, sm, vm, vm, vm, vm, vm, vm] + [any_spec] * 6,
        out_specs=[vm, vm, vm, any_spec],
        scratch_shapes=[
            pltpu.VMEM((width, 3 * d), bf),
            pltpu.VMEM((nz, 2, 2, n_rows, width), bf),
            pltpu.VMEM(w_o.shape, bf),
            pltpu.VMEM((n_req, n_tok, d), f32),
            pltpu.VMEM((n_req, n_tok, d), f32),
            pltpu.VMEM((n_req, old, d), bf),
            pltpu.VMEM((n_req, old, d), bf),
            pltpu.VMEM((n_req, old, 2 * d), bf),
            pltpu.VMEM((n_req, n_tok, d), bf),
            pltpu.VMEM((n_req, n_tok, 2 * d), bf),
            pltpu.VMEM((n_req, n_tok, d), f32),
            pltpu.VMEM((n_req, n_tok, 2 * d), f32),
            pltpu.VMEM((n_req, 4 * n_rows, d), bf),
            pltpu.VMEM((n_req, 4 * n_rows, d), f32),
            pltpu.VMEM((n_req, 4 * n_rows, 2 * d), f32),
            pltpu.VMEM((n_req, n_tok, d), bf),
            dma((4,)), dma((2,)), dma((nz, 2, STREAMS)), dma((nz, 2, STREAMS)), dma((nz, 2)), dma((nz, 2)),
            dma((nz, 2)), dma((nz, 2)), dma((nz, 2, n_dp)), dma((nz, 2, n_dp)), dma((nz, 2)), dma((nz, 2)),
            dma((nz, 2, 2)), dma((nz, 2, 2)),
        ],
        compiler_params=pltpu.CompilerParams(vmem_limit_bytes=62 * 2**20, collective_id=2, has_side_effects=True),
        cost_estimate=pl.CostEstimate(flops=8 * n_req * n_tok * slots * d, bytes_accessed=20 * 2**20, transcendentals=n_req * n_tok * slots),
        name="front",
    )(prefix, valid, x, gain, freq, b_q, b_k, b_v, w_q, w_k, w_v, w_o, k_cache, v_cache)


def merge_kernel(p_ref, c_ref, kn_hbm, vn_hbm, kc_hbm, vc_hbm, ko_hbm, vo_hbm, cache, fresh_rows, shift, sems, new_sem):
    n_req, n_tok, d = kn_hbm.shape
    slots = ko_hbm.shape[1]
    win = n_tok + 16
    olds, outs = (kc_hbm, vc_hbm), (ko_hbm, vo_hbm)
    new_in = [pltpu.make_async_copy(h, fresh_rows.at[i], new_sem.at[i]) for i, h in enumerate((kn_hbm, vn_hbm))]
    pairs = [(r, i) for r in range(n_req) for i in range(2)]
    moves_in = [pltpu.make_async_copy(olds[i].at[r], cache.at[r, i], sems.at[0, r, i]) for r, i in pairs]
    moves_out = [pltpu.make_async_copy(cache.at[r, i], outs[i].at[r], sems.at[1, r, i]) for r, i in pairs]
    for c in new_in + moves_in:
        c.start()
    for c in new_in:
        c.wait()
    for n, (r, i) in enumerate(pairs):
        start = pl.multiple_of(jnp.minimum((p_ref[r] // 16) * 16, slots - win), 16)
        off = p_ref[r] - start
        at = lax.broadcasted_iota(jnp.int32, (win, d), 0) - off
        fresh = (at >= 0) & (at < c_ref[r])
        shift[pl.ds(16, n_tok), :] = fresh_rows[i, r].astype(jnp.float32)
        moved = shift[pl.ds(16 - off, win), :]
        moves_in[n].wait()
        part = pl.ds(start, win)
        cache[r, i, part, :] = jnp.where(fresh, moved, cache[r, i, part, :].astype(jnp.float32)).astype(cache.dtype)
        moves_out[n].start()
    for c in moves_out:
        c.wait()


def merge(prefix, valid, k_new, v_new, k_cache, v_cache):
    n_req, n_tok, d = k_new.shape
    slots = k_cache.shape[1]
    any_spec = pl.BlockSpec(memory_space=pl.ANY)
    sm = pl.BlockSpec(memory_space=pltpu.SMEM)
    same = jax.ShapeDtypeStruct(k_cache.shape, k_cache.dtype)
    return pl.pallas_call(
        merge_kernel,
        out_shape=[same, same],
        in_specs=[sm, sm] + [any_spec] * 4,
        out_specs=[any_spec, any_spec],
        scratch_shapes=[
            pltpu.VMEM((n_req, 2, slots, d), k_cache.dtype),
            pltpu.VMEM((2, n_req, n_tok, d), k_new.dtype),
            pltpu.VMEM((n_tok + 32, d), jnp.float32),
            pltpu.SemaphoreType.DMA((2, n_req, 2)),
            pltpu.SemaphoreType.DMA((2,)),
        ],
        compiler_params=pltpu.CompilerParams(vmem_limit_bytes=62 * 2**20),
        cost_estimate=pl.CostEstimate(flops=10**6, bytes_accessed=16 * 2**20, transcendentals=0),
        name="merge",
    )(prefix, valid, k_new, v_new, k_cache, v_cache)


def solution(mesh):
    n_tp = mesh.shape["tp"]
    row_spec = P("dp", "tp", None)
    cache_spec = P("dp", None, "tp", None)
    req_spec = P("dp")
    rep_spec = P(None)
    col_spec = P(None, "tp")
    bias_spec = P("tp")
    down_spec = P("tp", None)

    def layer(x_rows, k_cache, v_cache, prefix, valid, g_attn, w_q, b_q, w_k, b_k, w_v, b_v, w_o, g_mlp, w_gate, w_up, w_down):
        n_req, head_dim = x_rows.shape[0], k_cache.shape[-1]
        half = np.arange(head_dim // 2, dtype=np.float32)
        freq = np.float32(ROPE_THETA) ** (-(half * np.float32(2.0)) / np.float32(head_dim))
        freq = jnp.asarray(np.concatenate([freq, freq])[None], jnp.float32)
        flat = (n_req, -1, head_dim)
        k_flat, v_flat = k_cache.reshape(flat), v_cache.reshape(flat)
        o, k_new, v_new, w_o_full = front(n_tp, mesh.shape["dp"], x_rows, g_attn, prefix, valid, freq, b_q, b_k, b_v, w_q, w_k, w_v, w_o, k_flat, v_flat)
        k_out, v_out = merge(prefix, valid, k_new, v_new, k_flat, v_flat)
        out = tail(n_tp, o, x_rows, g_mlp, w_o_full, w_gate.T, w_up.T, w_down)
        return out, k_out.reshape(k_cache.shape), v_out.reshape(v_cache.shape)

    in_specs = (row_spec, cache_spec, cache_spec, req_spec, req_spec, rep_spec, col_spec, bias_spec, col_spec, bias_spec, col_spec, bias_spec, down_spec, rep_spec, col_spec, col_spec, down_spec)
    return jax.shard_map(layer, mesh=mesh, in_specs=in_specs, out_specs=(row_spec, cache_spec, cache_spec), check_vma=False)
```

```python
import functools
import math

import jax
import jax.numpy as jnp
import numpy as np
from jax import lax
from jax.experimental import pallas as pl
from jax.experimental.pallas import tpu as pltpu
from jax.sharding import PartitionSpec as P

ROPE_THETA = 1.0e6
NORM_EPS = 1.0e-6


CHUNKS = 1
WO_BITES = 4
MESH = pl.DeviceIdType.MESH


def remote(src, dst, send, recv, target):
    return pltpu.make_async_remote_copy(src_ref=src, dst_ref=dst, send_sem=send, recv_sem=recv, device_id={"tp": target}, device_id_type=MESH)


def tail_kernel(n_tp, o_all, x_ref, g_ref, wo_hbm, wg_hbm, wu_hbm, wd_hbm, out_ref,
                wo, wg, wu, wd, x1, rows, sums_in, sums_out, part_in, part_out, kept,
                load_sem, bite_sem, ring_send, ring_recv, pair_send, pair_recv, sum_send, sum_recv, part_send, part_recv):
    nz = n_tp // 2
    me = lax.axis_index("tp")
    core = lax.rem(me, 2)
    chip = me // 2
    up = lax.rem(chip + 1, nz) * 2 + core
    down = lax.rem(chip + nz - 1, nz) * 2 + core
    pair = chip * 2 + 1 - core
    towards = (up, down)
    n_req, n_rows, width = x_ref.shape

    loads = [pltpu.make_async_copy(s, t, load_sem.at[i]) for i, (s, t) in enumerate(((wg_hbm, wg), (wu_hbm, wu), (wd_hbm, wd)))]
    bite = wo.shape[0] // WO_BITES
    bites = [pltpu.make_async_copy(wo_hbm.at[pl.ds(i * bite, bite)], wo.at[pl.ds(i * bite, bite)], bite_sem.at[i]) for i in range(WO_BITES)]
    for c in bites:
        c.start()

    barrier = pltpu.get_barrier_semaphore()
    for there in (up, down, pair):
        pl.semaphore_signal(barrier, inc=1, device_id={"tp": there}, device_id_type=MESH)

    heads = o_all[...].reshape(n_req * n_rows, width)
    mixed = None
    for i in range(WO_BITES):
        bites[i].wait()
        if i == WO_BITES - 1:
            for c in loads:
                c.start()
        at = slice(i * bite, (i + 1) * bite)
        piece = jnp.dot(heads[:, at], wo[at, :], preferred_element_type=jnp.float32)
        mixed = piece if mixed is None else mixed + piece
    mixed = mixed.astype(jnp.bfloat16)
    resid = (x_ref[...].reshape(n_req * n_rows, width).astype(jnp.float32) + mixed.astype(jnp.float32)).astype(jnp.bfloat16)
    x1[...] = resid.reshape(x1.shape)
    wide = resid.astype(jnp.float32)
    inv = lax.rsqrt(jnp.mean(wide * wide, axis=-1, keepdims=True) + NORM_EPS)
    normed = (wide * inv * g_ref[...].astype(jnp.float32).reshape(1, width)).astype(jnp.bfloat16)
    pl.semaphore_wait(barrier, 3)
    rows[0, :, 0] = normed.reshape(n_req, n_rows, width)

    for c in loads:
        c.wait()

    span = n_rows // CHUNKS

    def ring_copy(s, way, h):
        part = pl.ds(h * span, span)
        return remote(rows.at[s, way, 0, part], rows.at[s + 1, way, 0, part], ring_send.at[s, way, h], ring_recv.at[s + 1, way, h], towards[way])

    def pair_copy(s, way):
        return remote(rows.at[s, way, 0], rows.at[s, way, 1], pair_send.at[s, way], pair_recv.at[s, way], pair)

    def part_copy(s):
        return remote(part_out.at[s], part_in.at[s], part_send.at[s], part_recv.at[s], pair)

    def sum_copy(s, way, h):
        part = pl.ds(h * span, span)
        return remote(sums_out.at[s, way, part], sums_in.at[s + 1, way, part], sum_send.at[s, way, h], sum_recv.at[s + 1, way, h], towards[way])

    def step(s, _):
        for h in range(CHUNKS):
            for way in range(2):
                @pl.when(s > 0)
                def _():
                    ring_copy(s - 1, way, h).wait_recv()

                @pl.when(s < nz - 1)
                def _():
                    ring_copy(s, way, h).start()

        for way in range(2):
            pair_copy(s, way).start()
        for way in range(2):
            pair_copy(s, way).wait_recv()
        lhs = rows[s].reshape(4 * n_rows, width)
        gate = lax.dot_general(lhs, wg[...], (((1,), (1,)), ((), ())), preferred_element_type=jnp.float32)
        lift = lax.dot_general(lhs, wu[...], (((1,), (1,)), ((), ())), preferred_element_type=jnp.float32)
        act = (jax.nn.silu(gate) * lift).astype(jnp.bfloat16)
        part = jnp.dot(act, wd[...], preferred_element_type=jnp.float32).reshape(2, 2, n_rows, width)
        part_out[s] = part[:, 1].astype(jnp.bfloat16)
        part_copy(s).start()
        kept[jnp.minimum(s, 1)] = part[:, 0]

        @pl.when(s > 0)
        def _():
            part_copy(s).wait_recv()
            for h in range(CHUNKS):
                part = pl.ds(h * span, span)
                for way in range(2):
                    @pl.when(s > 1)
                    def _():
                        sum_copy(s - 1, way, h).wait_recv()
                        sums_out[s, way, part] = (kept[1, way, part] + part_in[s, way, part].astype(jnp.float32) + sums_in[s, way, part].astype(jnp.float32)).astype(jnp.bfloat16)

                    @pl.when(s == 1)
                    def _():
                        sums_out[s, way, part] = (kept[1, way, part] + part_in[s, way, part].astype(jnp.float32)).astype(jnp.bfloat16)

                    sum_copy(s, way, h).start()
        return 0

    lax.fori_loop(0, nz, step, 0)

    part_copy(0).wait_recv()
    for h in range(CHUNKS):
        part = pl.ds(h * span, span)
        for way in range(2):
            sum_copy(nz - 1, way, h).wait_recv()
            total = kept[0, way, part] + part_in[0, way, part].astype(jnp.float32) + sums_in[nz, way, part].astype(jnp.float32)
            out_ref[way, part] = (x1[way, part].astype(jnp.float32) + total.astype(jnp.bfloat16).astype(jnp.float32)).astype(jnp.bfloat16)

    for s in range(nz):
        part_copy(s).wait_send()
        for way in range(2):
            pair_copy(s, way).wait_send()
            if s < nz - 1:
                for h in range(CHUNKS):
                    ring_copy(s, way, h).wait_send()
            if s > 0:
                for h in range(CHUNKS):
                    sum_copy(s, way, h).wait_send()


def tail(n_tp, o, x, gain, w_o, w_gate, w_up, w_down):
    n_req, n_rows, width = x.shape
    ffn = w_gate.shape[0]
    nz = n_tp // 2
    bf = jnp.bfloat16
    any_spec = pl.BlockSpec(memory_space=pl.ANY)
    vm = pl.BlockSpec(memory_space=pltpu.VMEM)
    dma = pltpu.SemaphoreType.DMA
    return pl.pallas_call(
        functools.partial(tail_kernel, n_tp),
        out_shape=jax.ShapeDtypeStruct(x.shape, x.dtype),
        in_specs=[vm, vm, vm, any_spec, any_spec, any_spec, any_spec],
        out_specs=vm,
        scratch_shapes=[
            pltpu.VMEM(w_o.shape, bf),
            pltpu.VMEM(w_gate.shape, bf),
            pltpu.VMEM(w_up.shape, bf),
            pltpu.VMEM(w_down.shape, bf),
            pltpu.VMEM((n_req, n_rows, width), bf),
            pltpu.VMEM((nz, 2, 2, n_rows, width), bf),
            pltpu.VMEM((nz + 1, 2, n_rows, width), bf),
            pltpu.VMEM((nz, 2, n_rows, width), bf),
            pltpu.VMEM((nz, 2, n_rows, width), bf),
            pltpu.VMEM((nz, 2, n_rows, width), bf),
            pltpu.VMEM((2, 2, n_rows, width), jnp.float32),
            dma((3,)), dma((WO_BITES,)),
            dma((nz, 2, CHUNKS)), dma((nz, 2, CHUNKS)), dma((nz, 2)), dma((nz, 2)),
            dma((nz, 2, CHUNKS)), dma((nz + 1, 2, CHUNKS)), dma((nz,)), dma((nz,)),
        ],
        compiler_params=pltpu.CompilerParams(vmem_limit_bytes=62 * 2**20, collective_id=1, has_side_effects=True),
        cost_estimate=pl.CostEstimate(flops=6 * n_tp * n_req * n_rows * width * ffn, bytes_accessed=20 * 2**20, transcendentals=0),
        name="tail",
    )(o, x, gain, w_o, w_gate, w_up, w_down)


NEG = -1.0e30
KEY_BLOCKS = 4
STREAMS = 2


def front_kernel(n_tp, n_dp, p_ref, c_ref, x_ref, g_ref, f_ref, bq_ref, bk_ref, bv_ref, wq_hbm, wk_hbm, wv_hbm, wo_hbm, kc_hbm, vc_hbm,
                 o_all, kn_ref, vn_ref, all_hbm,
                 w, rows, wo, cos_v, sin_v, kc, vc, vext, q_abs, vn_ext, m_abs, acc_abs, q_now, m_now, acc_now, o_v,
                 load_sem, cache_sem, ring_send, ring_recv, pair_send, pair_recv, a_send, a_recv, b_send, b_recv, c_send, c_recv, o_send, o_recv):
    nz = n_tp // 2
    me = lax.axis_index("tp")
    core = lax.rem(me, 2)
    chip = me // 2
    group = lax.axis_index("dp")
    up = lax.rem(chip + 1, nz) * 2 + core
    down = lax.rem(chip + nz - 1, nz) * 2 + core
    pair = chip * 2 + 1 - core
    towards = (up, down)
    n_req, n_rows, width = x_ref.shape
    d = q_abs.shape[-1]
    two = 2 * n_rows
    old = vext.shape[1]
    bf, f32 = jnp.bfloat16, jnp.float32

    own_load = pltpu.make_async_copy(wo_hbm, wo, load_sem.at[3])
    own_load.start()
    loads = [pltpu.make_async_copy(s, w.at[:, pl.ds(i * d, d)], load_sem.at[i]) for i, s in enumerate((wq_hbm, wk_hbm, wv_hbm))]
    for c in loads:
        c.start()
    cache_in = [pltpu.make_async_copy(s.at[:, pl.ds(0, old)], t, cache_sem.at[i]) for i, (s, t) in enumerate(((kc_hbm, kc), (vc_hbm, vc)))]
    for c in cache_in:
        c.start()

    barrier = pltpu.get_barrier_semaphore()
    for k in range(1, n_tp):
        pl.semaphore_signal(barrier, inc=1, device_id={"tp": lax.rem(me + k, n_tp)}, device_id_type=MESH)
    for k in range(1, n_dp):
        pl.semaphore_signal(barrier, inc=1, device_id={"dp": lax.rem(group + k, n_dp)}, device_id_type=MESH)

    wide = x_ref[...].astype(f32)
    inv = lax.rsqrt(jnp.mean(wide * wide, axis=-1, keepdims=True) + NORM_EPS)
    rows[0, :, 0] = (wide * inv * g_ref[...].astype(f32).reshape(1, width)).astype(bf)
    pl.semaphore_wait(barrier, n_tp + n_dp - 2)

    span = n_rows // STREAMS

    def ring_copy(s, way, h):
        part = pl.ds(pl.multiple_of(h * span, span), span)
        return remote(rows.at[s, way, 0, part], rows.at[s + 1, way, 0, part], ring_send.at[s, way, h], ring_recv.at[s + 1, way, h], towards[way])

    def pair_copy(s, way):
        return remote(rows.at[s, way, 0], rows.at[s, way, 1], pair_send.at[s, way], pair_recv.at[s, way], pair)

    n_own = wo.shape[0]
    share = n_own // n_dp
    reach = (nz // 2, (nz - 1) // 2)

    def away(s, way):
        return lax.rem(chip + (nz - s if way == 0 else s), nz)

    def home_rows(s, way, part, count):
        return pl.ds(pl.multiple_of((away(s, way) * 2 + core) * n_own + part * share, 8), count)

    def a_copy(s, way, src=None):
        at = home_rows(s, way, group, share)
        return remote(all_hbm.at[at] if src is None else src, all_hbm.at[at], a_send.at[s, way], a_recv.at[s + 1, way], towards[way])

    def b_copy(s, way, k, owner=None):
        at = home_rows(s, way, group if owner is None else owner, share)
        return pltpu.make_async_remote_copy(src_ref=all_hbm.at[at], dst_ref=all_hbm.at[at], send_sem=b_send.at[s, way, k], recv_sem=b_recv.at[s, way, k],
                                            device_id={"dp": lax.rem(group + k, n_dp)}, device_id_type=MESH)

    def c_copy(s, way, src=None):
        at = home_rows(s, way, 0, n_own)
        return remote(all_hbm.at[at] if src is None else src, all_hbm.at[at], c_send.at[s, way], c_recv.at[s, way], pair)

    def c_wait(s, way):
        at = pl.ds(pl.multiple_of((away(s, way) * 2 + 1 - core) * n_own, 8), n_own)
        remote(all_hbm.at[at], all_hbm.at[at], c_send.at[s, way], c_recv.at[s, way], pair).wait_recv()

    for h in range(STREAMS):
        for way in range(2):
            ring_copy(0, way, h).start()
    for way in range(2):
        pair_copy(0, way).start()
    own_load.wait()
    own_share = wo.at[pl.ds(pl.multiple_of(group * share, 8), share)]
    own_store = pltpu.make_async_copy(wo, all_hbm.at[home_rows(0, 0, 0, n_own)], load_sem.at[3])
    for way in range(2):
        a_copy(0, way, own_share).start()
    own_store.start()
    c_copy(0, 0, wo).start()

    for c in cache_in:
        c.wait()
    tile = 1024
    for r in range(n_req):
        def tidy(t, _):
            at = pl.ds(pl.multiple_of(t * tile, tile), tile)
            there = lax.broadcasted_iota(jnp.int32, (tile, d), 0) + t * tile < p_ref[r]
            first = kc[r, 0:16, :].astype(f32)[0:1]
            kc[r, at, :] = jnp.where(there, kc[r, at, :].astype(f32), first).astype(bf)
            vext[r, at, :d] = jnp.where(there, vc[r, at, :].astype(f32), 0.0).astype(bf)
            vext[r, at, d:] = jnp.where(there, 1.0, 0.0).astype(bf)
            return 0

        lax.fori_loop(0, old // tile, tidy, 0)
    turn = 128
    sign = jnp.where(lax.broadcasted_iota(jnp.int32, (turn, d), 1) < d // 2, -1.0, 1.0)
    for r in range(n_req):
        def angles(t, _):
            spot = (lax.broadcasted_iota(jnp.int32, (turn, d), 0) + (p_ref[r] + t * turn)).astype(f32)
            angle = spot * f_ref[...]
            at = pl.ds(pl.multiple_of(t * turn, turn), turn)
            cos_v[r, at, :] = jnp.cos(angle)
            sin_v[r, at, :] = jnp.sin(angle) * sign
            return 0

        lax.fori_loop(0, cos_v.shape[1] // turn, angles, 0)
    vn_ext[:, :, d:] = jnp.ones((n_req, vn_ext.shape[1], d), bf)
    for c in loads:
        c.wait()

    def pass_on(s, h):
        @pl.when(s < nz)
        def _():
            for way in range(2):
                ring_copy(s - 1, way, h).wait_recv()

                @pl.when(s < nz - 1)
                def _():
                    ring_copy(s, way, h).start()

    def landed(s):
        @pl.when(s < nz)
        def _():
            for way in range(2):
                pair_copy(s, way).start()

                @pl.when(s <= reach[way])
                def _():
                    a_copy(s - 1, way).wait_recv()

                    @pl.when(s < reach[way])
                    def _():
                        a_copy(s, way).start()

                    for k in range(1, n_dp):
                        b_copy(s, way, k).start()

    scale2 = (d ** -0.5) * math.log2(math.e)
    block = old // KEY_BLOCKS
    nt = (((1,), (1,)), ((), ()))

    def flash(s, m_prev, acc, vals):
        m_new = jnp.maximum(m_prev, jnp.max(s, axis=1, keepdims=True))
        a = jnp.exp2((m_prev - m_new) * scale2)
        p = jnp.exp2((s - m_new[:, :1]) * scale2).astype(bf)
        return m_new, acc * jnp.concatenate([a, a], axis=1) + jnp.dot(p, vals, preferred_element_type=f32)

    for h in range(STREAMS):
        pass_on(1, h)
    landed(1)

    def places(k):
        for t in range(2):
            for way in range(2):
                for other in range(2):
                    off = pl.multiple_of((away(2 * k + t, way) * 2 + (core if other == 0 else 1 - core)) * n_rows, n_rows)
                    yield t, way, other, off

    def project(k):
        for t in range(2):
            for way in range(2):
                pair_copy(2 * k + t, way).wait_recv()
        lhs = rows[pl.ds(2 * k, 2)].reshape(8 * n_rows, width)
        total = jnp.dot(lhs, w[...], preferred_element_type=f32)
        got = [(total[:, i * d:(i + 1) * d] + b[...].astype(f32).reshape(1, d)).astype(bf) for i, b in enumerate((bq_ref, bk_ref, bv_ref))]

        for t, way, other, off in places(k):
            at = pl.ds(off, n_rows)
            cos_t, sin_t = cos_v[way, at, :], sin_v[way, at, :]
            i = ((t * 2 + way) * 2 + other) * n_rows
            turned = []
            for part in got[:2]:
                part = part[i:i + n_rows].astype(f32)
                turned.append((part * cos_t + pltpu.roll(part, d // 2, 1) * sin_t).astype(bf))
            q_abs[way, at, :] = turned[0]
            q_now[way, pl.ds(t * two + other * n_rows, n_rows), :] = turned[0]
            kn_ref[way, at, :] = turned[1]
            vn_ref[way, at, :] = got[2][i:i + n_rows]
            vn_ext[way, at, :d] = got[2][i:i + n_rows]

    def attend_old(k, ticks):
        m_now[...] = jnp.full_like(m_now, NEG)
        acc_now[...] = jnp.zeros_like(acc_now)

        def keys(j, _):
            at = pl.ds(pl.multiple_of(j * block, block), block)
            for u in range(2):
                for way in range(2):
                    sl = pl.ds(u * two, two)
                    s = lax.dot_general(q_now[way, sl, :], kc[way, at, :], nt, preferred_element_type=f32)
                    m_now[way, sl, :], acc_now[way, sl, :] = flash(s, m_now[way, sl, :], acc_now[way, sl, :], vext[way, at, :])

            if ticks:
                for n in range(2 * STREAMS // KEY_BLOCKS):
                    event = j * (2 * STREAMS // KEY_BLOCKS) + n
                    step = 2 * k + 2 + event // STREAMS
                    pass_on(step, lax.rem(event, STREAMS))

                    @pl.when(lax.rem(event, STREAMS) == STREAMS - 1)
                    def _():
                        landed(step)
            return 0

        lax.fori_loop(0, KEY_BLOCKS, keys, 0)
        for t, way, other, off in places(k):
            at = pl.ds(off, n_rows)
            here = pl.ds(t * two + other * n_rows, n_rows)
            m_abs[way, at, :] = m_now[way, here, :]
            acc_abs[way, at, :] = acc_now[way, here, :]

    def two_steps(k, _):
        project(k)
        attend_old(k, True)
        return 0

    last = nz // 2 - 1
    lax.fori_loop(0, last, two_steps, 0)
    project(last)

    pieces = [(s, way) for s in range(1, nz // 2 + 1) for way in range(2) if s <= reach[way]]
    for s, way in pieces:
        for k in range(1, n_dp):
            b_copy(s, way, k, lax.rem(group + n_dp - k, n_dp)).wait_recv()
        c_copy(s, way).start()

    mine = pl.ds(pl.multiple_of(me * d, d), d)

    def o_copy(s, way, to):
        home = away(s, way)
        off = pl.multiple_of(home * two + to * n_rows, n_rows)
        return remote(o_v.at[way, pl.ds(off, n_rows), :], o_all.at[way, :, mine], o_send.at[s, way, to], o_recv.at[s, way, core], home * 2 + to)

    def finish(i, _):
        for way in range(2):
            home = away(i, way)
            at = pl.ds(pl.multiple_of(home * two, two), two)
            s = lax.dot_general(q_abs[way, at, :], kn_ref[way], nt, preferred_element_type=f32)
            rid = lax.broadcasted_iota(jnp.int32, (two, 1), 0) + home * two
            s = jnp.where(lax.broadcasted_iota(jnp.int32, s.shape, 1) <= jnp.minimum(rid, c_ref[way] - 1), s, NEG)
            m_prev = jnp.where(jnp.full((two, d), p_ref[way], jnp.int32) > 0, m_abs[way, at, :], NEG)
            _, acc = flash(s, m_prev, acc_abs[way, at, :], vn_ext[way])
            o_v[way, at, :] = (acc[:, :d] / acc[:, d:]).astype(bf)
        for way in range(2):
            for to in range(2):
                @pl.when((i > 0) | (core != to))
                def _():
                    o_copy(i, way, to).start()

                @pl.when((i == 0) & (core == to))
                def _():
                    o_all[way, :, mine] = o_v[way, pl.ds(pl.multiple_of(chip * two + to * n_rows, n_rows), n_rows), :]
        return 0

    lax.fori_loop(0, 2 * last, finish, 0)
    attend_old(last, False)
    lax.fori_loop(2 * last, nz, finish, 0)

    def o_wait(i, _):
        for way in range(2):
            for to in range(2):
                @pl.when((i > 0) | (core != to))
                def _():
                    source = away(i, 1 - way) * 2 + to
                    spot = pl.ds(pl.multiple_of(source * d, d), d)
                    remote(o_v.at[way, pl.ds(0, n_rows), :], o_all.at[way, :, spot], o_send.at[i, way, to], o_recv.at[i, way, to], pair).wait_recv()
                    o_copy(i, way, to).wait_send()
        return 0

    lax.fori_loop(0, nz, o_wait, 0)

    own_store.wait()
    c_copy(0, 0, wo).wait_send()
    c_wait(0, 0)
    for way in range(2):
        a_copy(0, way, own_share).wait_send()
    for s, way in pieces:
        c_wait(s, way)
        c_copy(s, way).wait_send()
        for k in range(1, n_dp):
            b_copy(s, way, k).wait_send()
        if s < reach[way]:
            a_copy(s, way).wait_send()
    for s in range(nz):
        for way in range(2):
            pair_copy(s, way).wait_send()
            if s < nz - 1:
                for h in range(STREAMS):
                    ring_copy(s, way, h).wait_send()


def front(n_tp, n_dp, x, gain, prefix, valid, freq, b_q, b_k, b_v, w_q, w_k, w_v, w_o, k_cache, v_cache):
    n_req, n_rows, width = x.shape
    d = w_q.shape[1]
    nz = n_tp // 2
    n_tok = n_rows * n_tp
    slots = k_cache.shape[1]
    old = slots - n_tok
    bf, f32 = jnp.bfloat16, jnp.float32
    any_spec = pl.BlockSpec(memory_space=pl.ANY)
    sm = pl.BlockSpec(memory_space=pltpu.SMEM)
    vm = pl.BlockSpec(memory_space=pltpu.VMEM)
    dma = pltpu.SemaphoreType.DMA
    made = jax.ShapeDtypeStruct((n_req, n_tok, d), bf)
    return pl.pallas_call(
        functools.partial(front_kernel, n_tp, n_dp),
        out_shape=[jax.ShapeDtypeStruct(x.shape, bf), made, made, jax.ShapeDtypeStruct((n_tp * d, width), bf)],
        in_specs=[sm, sm, vm, vm, vm, vm, vm, vm] + [any_spec] * 6,
        out_specs=[vm, vm, vm, any_spec],
        scratch_shapes=[
            pltpu.VMEM((width, 3 * d), bf),
            pltpu.VMEM((nz, 2, 2, n_rows, width), bf),
            pltpu.VMEM(w_o.shape, bf),
            pltpu.VMEM((n_req, n_tok, d), f32),
            pltpu.VMEM((n_req, n_tok, d), f32),
            pltpu.VMEM((n_req, old, d), bf),
            pltpu.VMEM((n_req, old, d), bf),
            pltpu.VMEM((n_req, old, 2 * d), bf),
            pltpu.VMEM((n_req, n_tok, d), bf),
            pltpu.VMEM((n_req, n_tok, 2 * d), bf),
            pltpu.VMEM((n_req, n_tok, d), f32),
            pltpu.VMEM((n_req, n_tok, 2 * d), f32),
            pltpu.VMEM((n_req, 4 * n_rows, d), bf),
            pltpu.VMEM((n_req, 4 * n_rows, d), f32),
            pltpu.VMEM((n_req, 4 * n_rows, 2 * d), f32),
            pltpu.VMEM((n_req, n_tok, d), bf),
            dma((4,)), dma((2,)), dma((nz, 2, STREAMS)), dma((nz, 2, STREAMS)), dma((nz, 2)), dma((nz, 2)),
            dma((nz, 2)), dma((nz, 2)), dma((nz, 2, n_dp)), dma((nz, 2, n_dp)), dma((nz, 2)), dma((nz, 2)),
            dma((nz, 2, 2)), dma((nz, 2, 2)),
        ],
        compiler_params=pltpu.CompilerParams(vmem_limit_bytes=62 * 2**20, collective_id=2, has_side_effects=True),
        cost_estimate=pl.CostEstimate(flops=8 * n_req * n_tok * slots * d, bytes_accessed=20 * 2**20, transcendentals=n_req * n_tok * slots),
        name="front",
    )(prefix, valid, x, gain, freq, b_q, b_k, b_v, w_q, w_k, w_v, w_o, k_cache, v_cache)


def merge_kernel(p_ref, c_ref, x_hbm, kn_hbm, vn_hbm, kc_hbm, vc_hbm, xo_hbm, ko_hbm, vo_hbm, x_v, cache, fresh_rows, shift, sems, new_sem, x_sem):
    n_req, n_tok, d = kn_hbm.shape
    slots = ko_hbm.shape[1]
    win = n_tok + 16
    olds, outs = (kc_hbm, vc_hbm), (ko_hbm, vo_hbm)
    new_in = [pltpu.make_async_copy(h, fresh_rows.at[i], new_sem.at[i]) for i, h in enumerate((kn_hbm, vn_hbm))]
    pairs = [(r, i) for r in range(n_req) for i in range(2)]
    moves_in = [pltpu.make_async_copy(olds[i].at[r], cache.at[r, i], sems.at[0, r, i]) for r, i in pairs]
    moves_out = [pltpu.make_async_copy(cache.at[r, i], outs[i].at[r], sems.at[1, r, i]) for r, i in pairs]
    x_in = pltpu.make_async_copy(x_hbm, x_v, x_sem.at[0])
    x_out = pltpu.make_async_copy(x_v, xo_hbm, x_sem.at[1])
    for c in new_in + [x_in] + moves_in:
        c.start()
    for c in new_in:
        c.wait()
    x_in.wait()
    x_out.start()
    for n, (r, i) in enumerate(pairs):
        start = pl.multiple_of(jnp.minimum((p_ref[r] // 16) * 16, slots - win), 16)
        off = p_ref[r] - start
        at = lax.broadcasted_iota(jnp.int32, (win, d), 0) - off
        fresh = (at >= 0) & (at < c_ref[r])
        shift[pl.ds(16, n_tok), :] = fresh_rows[i, r].astype(jnp.float32)
        moved = shift[pl.ds(16 - off, win), :]
        moves_in[n].wait()
        part = pl.ds(start, win)
        cache[r, i, part, :] = jnp.where(fresh, moved, cache[r, i, part, :].astype(jnp.float32)).astype(cache.dtype)
        moves_out[n].start()
    for c in moves_out:
        c.wait()
    x_out.wait()


def merge(prefix, valid, x_new, k_new, v_new, k_cache, v_cache):
    n_req, n_tok, d = k_new.shape
    slots = k_cache.shape[1]
    any_spec = pl.BlockSpec(memory_space=pl.ANY)
    sm = pl.BlockSpec(memory_space=pltpu.SMEM)
    same = jax.ShapeDtypeStruct(k_cache.shape, k_cache.dtype)
    return pl.pallas_call(
        merge_kernel,
        out_shape=[jax.ShapeDtypeStruct(x_new.shape, x_new.dtype), same, same],
        in_specs=[sm, sm] + [any_spec] * 5,
        out_specs=[any_spec] * 3,
        scratch_shapes=[
            pltpu.VMEM(x_new.shape, x_new.dtype),
            pltpu.VMEM((n_req, 2, slots, d), k_cache.dtype),
            pltpu.VMEM((2, n_req, n_tok, d), k_new.dtype),
            pltpu.VMEM((n_tok + 32, d), jnp.float32),
            pltpu.SemaphoreType.DMA((2, n_req, 2)),
            pltpu.SemaphoreType.DMA((2,)),
            pltpu.SemaphoreType.DMA((2,)),
        ],
        compiler_params=pltpu.CompilerParams(vmem_limit_bytes=62 * 2**20),
        cost_estimate=pl.CostEstimate(flops=10**6, bytes_accessed=16 * 2**20, transcendentals=0),
        name="merge",
    )(prefix, valid, x_new, k_new, v_new, k_cache, v_cache)


def solution(mesh):
    n_tp = mesh.shape["tp"]
    row_spec = P("dp", "tp", None)
    cache_spec = P("dp", None, "tp", None)
    req_spec = P("dp")
    rep_spec = P(None)
    col_spec = P(None, "tp")
    bias_spec = P("tp")
    down_spec = P("tp", None)

    def layer(x_rows, k_cache, v_cache, prefix, valid, g_attn, w_q, b_q, w_k, b_k, w_v, b_v, w_o, g_mlp, w_gate, w_up, w_down):
        n_req, head_dim = x_rows.shape[0], k_cache.shape[-1]
        half = np.arange(head_dim // 2, dtype=np.float32)
        freq = np.float32(ROPE_THETA) ** (-(half * np.float32(2.0)) / np.float32(head_dim))
        freq = jnp.asarray(np.concatenate([freq, freq])[None], jnp.float32)
        flat = (n_req, -1, head_dim)
        k_flat, v_flat = k_cache.reshape(flat), v_cache.reshape(flat)
        o, k_new, v_new, w_o_full = front(n_tp, mesh.shape["dp"], x_rows, g_attn, prefix, valid, freq, b_q, b_k, b_v, w_q, w_k, w_v, w_o, k_flat, v_flat)
        out = tail(n_tp, o, x_rows, g_mlp, w_o_full, w_gate.T, w_up.T, w_down)
        out, k_out, v_out = merge(prefix, valid, out, k_new, v_new, k_flat, v_flat)
        return out, k_out.reshape(k_cache.shape), v_out.reshape(v_cache.shape)

    in_specs = (row_spec, cache_spec, cache_spec, req_spec, req_spec, rep_spec, col_spec, bias_spec, col_spec, bias_spec, col_spec, bias_spec, down_spec, rep_spec, col_spec, col_spec, down_spec)
    return jax.shard_map(layer, mesh=mesh, in_specs=in_specs, out_specs=(row_spec, cache_spec, cache_spec), check_vma=False)
```
